128 devices in a mesh: px: 8 (over y, x_lo), py: 16 (over z, x_hi, core).
Axes of the slice: x: 4 (x_hi: 2, x_lo: 2; x = x_hi * 2 + x_lo), y: 4, z: 4, core: 2. Of those that a mesh axis runs over, the one named last changes fastest.
Arguments:
- coefficients: bfloat16 [1536, 49152], P(('px', 'py')), may hold values from -6 to 6
- exponents: int32 [384, 3072], P(('px', 'py')), may hold values from -4 to 1
- right_side: float32 [128, 384, 1536], P('px', 'py'), may hold values from -18 to 18
Outputs:
- decoded: float32 [128, 384, 1536], P('px', 'py')
- residual: float32 [128, 384, 1536], P('px', 'py')
- rms: float32 [], replicated
The draws below stay inside these ranges and needn't reach their ends.
All inputs are finite; a program needn't handle non-finite values.
Results may differ from the reference program's by a relative error of at most 0.0003.
Values may be sent and summed in bfloat16 or wider, within the bound.
A program may use at most 64 MiB of HBM per device.

```python
import jax
import jax.numpy as jnp
from jax import lax

CX = 16
CY = 24
BX = 32
BY = 96
BZ = 384
NX = 128
NY = 384
NZ = 1536


def draw_exponents(key, part):
    block_x = CX // 4
    block_y = CY // 4
    pencil_x = BX // block_x
    pencil_y = BY // block_y
    drawn_levels = jax.random.randint(key, (BZ, pencil_x, pencil_y, block_x, block_y), -3, 1)
    across_x = jnp.arange(pencil_x, dtype=jnp.int32)[:, None] * block_x + jnp.arange(block_x, dtype=jnp.int32)[None, :]
    across_y = jnp.arange(pencil_y, dtype=jnp.int32)[:, None] * block_y + jnp.arange(block_y, dtype=jnp.int32)[None, :]
    slope_x = (2 * across_x // BX)[None, :, None, :, None]
    slope_y = (2 * across_y // BY)[None, None, :, None, :]
    levels = drawn_levels + slope_x + slope_y - 1
    return levels.reshape(BZ, BX * BY).astype(jnp.int32)


def draw_right_side(key, part):
    first_key, second_key = jax.random.split(jax.random.fold_in(key, 7))
    column_scale = 0.3 * jnp.exp(jax.random.uniform(first_key, (NX, NY, 1), jnp.float32) * jnp.log(10.0))
    entries = jax.random.truncated_normal(second_key, -6.0, 6.0, (NX, NY, NZ), jnp.float32)
    return (entries * column_scale).astype(jnp.float32)


def block_scale(own_key, extent, cuts, smallest, largest):
    def one(position, blocks):
        steps = jax.random.uniform(jax.random.fold_in(jax.random.fold_in(own_key, 6), position), (blocks,), jnp.float32, smallest / len(cuts), largest / len(cuts))
        return jnp.repeat(jnp.exp(steps), extent[position] // blocks).reshape((-1,) + (1,) * (len(extent) - position - 1))

    loudness = one(*cuts[0])
    for cut in cuts[1:]:
        loudness = loudness * one(*cut)
    return loudness


def bell_draw(key, shape, scale, reach, cuts=(), kind=jnp.bfloat16):
    values = scale * jax.random.normal(key, shape, jnp.float32)
    if cuts:
        values = values * block_scale(key, shape, cuts, -0.22, 0.18)
    return jnp.clip(values, -reach, reach).astype(kind)


def setup_inputs(seed: int = 0) -> dict:
    streams_of = jax.random.split(jax.random.key(seed), 4)
    coefficients = bell_draw(streams_of[0], (NZ, NX * NY), 1.0, 6.0, ((0, 128),))
    exponents = draw_exponents(jax.random.fold_in(streams_of[3], 71), 0)
    right_side = draw_right_side(jax.random.fold_in(streams_of[3], 71), 0)
    return dict(coefficients=coefficients, exponents=exponents, right_side=right_side)


def basis_rows():
    points = jnp.arange(4, dtype=jnp.float32)
    frequency = points[:, None]
    cosine = jnp.cos(jnp.pi * (2.0 * points[None, :] + 1.0) * frequency / 8.0)
    weight = jnp.where(frequency == 0, jnp.sqrt(jnp.float32(0.25)), jnp.sqrt(jnp.float32(0.5)))
    return (weight * cosine).astype(jnp.float32)

def reference(coefficients, exponents, right_side):
    basis = basis_rows()
    pencil_x = NX // CX
    pencil_y = NY // CY
    held = coefficients.reshape(NZ, pencil_x, pencil_y, CX, CY).transpose(1, 3, 2, 4, 0).reshape(NX, NY, NZ)
    power = exponents.reshape(BZ, pencil_x, pencil_y, CX // 4, CY // 4).transpose(1, 3, 2, 4, 0).reshape(BX, BY, BZ)
    factor = jnp.exp2(power.astype(jnp.float32))
    factor = jnp.repeat(jnp.repeat(jnp.repeat(factor, 4, axis=0), 4, axis=1), 4, axis=2)
    scaled = (held.astype(jnp.float32) * factor).astype(jnp.bfloat16)
    blocks = scaled.astype(jnp.float32).reshape(BX, 4, BY, 4, BZ, 4)
    blocks = jnp.einsum('xaybzc,ai->xiybzc', blocks, basis, precision=lax.Precision.HIGHEST)
    blocks = jnp.einsum('xiybzc,bj->xiyjzc', blocks, basis, precision=lax.Precision.HIGHEST)
    blocks = jnp.einsum('xiyjzc,ck->xiyjzk', blocks, basis, precision=lax.Precision.HIGHEST)
    decoded = blocks.reshape(NX, NY, NZ)
    padded = jnp.pad(decoded, 1)
    beside = padded[2:, 1:-1, 1:-1] + padded[:-2, 1:-1, 1:-1]
    beside = beside + padded[1:-1, 2:, 1:-1] + padded[1:-1, :-2, 1:-1]
    beside = beside + padded[1:-1, 1:-1, 2:] + padded[1:-1, 1:-1, :-2]
    residual = right_side - (6.0 * decoded - beside)
    total_sum = jnp.sum(residual * residual)
    rms = jnp.sqrt(total_sum / (NX * NY * NZ) + 1e-06)
    return (decoded, residual, rms)
```

```python
import functools

import jax
import jax.numpy as jnp
import numpy as np
from jax import lax
from jax.experimental import pallas as pl
from jax.experimental.pallas import tpu as pltpu
from jax.sharding import PartitionSpec as P

CX = 16
CY = 24
CELLS = CX * CY
NZ = 1536
PEERS = 128
LAYERS = 12
ROWS = 16
F32 = jnp.float32
BF16 = jnp.bfloat16
MESH = pl.DeviceIdType.MESH


def basis():
    a = np.arange(4.0)[:, None]
    i = np.arange(4.0)[None, :]
    weight = np.where(a == 0, np.sqrt(0.25), np.sqrt(0.5))
    return weight * np.cos(np.pi * (2 * i + 1) * a / 8)


def halves(table):
    hi = table.astype(np.float32).astype(BF16)
    lo = (table - hi.astype(np.float64)).astype(np.float32).astype(BF16)
    return hi, lo


def block_table(width):
    b = basis()
    n = np.arange(width)
    return np.where(n[:, None] // 4 == n[None, :] // 4, b[n[:, None] % 4, n[None, :] % 4], 0.0)


def tables():
    b = basis()
    plane = np.kron(block_table(CX), block_table(CY))
    plane_hi, plane_lo = halves(plane.T)
    lane_of = np.zeros((3, 64), np.int64)
    cell_of = np.zeros(256, np.int64)
    part_of = np.full(256, -1)
    for k in range(3):
        for e in range(64):
            lane_of[k, e] = k * 48 + e if e < 48 else 144 + k * 16 + e - 48
        for e in range(24):
            cell_of[k * 48 + e] = e
            cell_of[k * 48 + 24 + e] = 15 * CY + e
        for x in range(16):
            cell_of[144 + k * 16 + x] = x * CY
            cell_of[192 + k * 16 + x] = x * CY + 23
        for first, size in ((k * 48, 48), (144 + k * 16, 16), (192 + k * 16, 16)):
            part_of[first : first + size] = k
    edge = np.where(part_of[None, :] >= 0, plane[:, cell_of], 0.0)
    edge_hi, edge_lo = halves(edge)
    keep = (np.arange(ROWS)[:, None] // 4 == part_of[None, :]).astype(np.float32)
    mix = np.zeros((256, 256))
    for p in range(16):
        q = p + 1 if p % 2 else p - 1
        for r in range(4):
            for z in range(LAYERS):
                mix[p * 8 + 4 + r, p * 16 + z] = b[z % 4, r]
                if 0 <= q < 16:
                    mix[128 + p * 8 + 4 + r, q * 16 + z] = b[z % 4, r]
    mix_hi, mix_lo = halves(mix)
    pick = np.zeros((192, CELLS))
    for k in range(3):
        for e in range(64):
            pick[k * 64 + e, lane_of[k, e]] = 1
            pick[k * 64 + e, 192 + lane_of[k, e]] = 1
    left = np.concatenate([plane_hi, plane_lo, pick.astype(BF16)], axis=0)
    depth = np.zeros((2, 256, 256))
    place = np.zeros((2, 768, 256))
    for odd in range(2):
        for s in range(16):
            base = 64 * odd + s * LAYERS
            for z in range(LAYERS):
                for o in range(z // 4 * 4, z // 4 * 4 + 4):
                    depth[odd, s * 16 + z, base + o] = b[z % 4, o % 4]
            for k in range(3):
                for r in range(4):
                    place[odd, k * 256 + s * 16 + 12 + r, base + k * 4 + r] = 1
    depth_hi, depth_lo = halves(depth)
    column = np.arange(CELLS)
    spread = (column[:, None] % 24 == (column[None, :] // CY // 4) * 6 + column[None, :] % CY // 4).astype(BF16)
    return (
        spread,
        np.stack([edge_hi, edge_lo]),
        keep,
        np.stack([mix_hi, mix_lo]),
        left,
        np.stack([depth_hi, depth_lo], axis=1),
        place.astype(BF16),
    )


def dot(a, b):
    return lax.dot_general(a, b, (((1,), (0,)), ((), ())), preferred_element_type=F32)


def dot_rows(a, b):
    return lax.dot_general(a, b, (((1,), (1,)), ((), ())), preferred_element_type=F32)


def two(x):
    hi = x.astype(BF16)
    return hi, (x - hi.astype(F32)).astype(BF16)


def position():
    i, j = lax.axis_index("px"), lax.axis_index("py")
    return (j // 2) % 2 * 2 + i % 2, i // 2, j // 4, j % 2


def device_at(x, y, z, c):
    return lax.rem(y, 4) * 2 + lax.rem(x, 2), lax.rem(z, 4) * 4 + lax.rem(x, 4) // 2 * 2 + lax.rem(c, 2)


def beside(dx, dy, dz, dc):
    x, y, z, c = position()
    return device_at(x + dx, y + dy, z + dz, c + dc)


def ident(pair):
    return {"px": pair[0], "py": pair[1]}


def kernel(
    coef_hbm, expo_hbm, right_hbm, spread_hbm, edge_hbm, keep_hbm, mix_hbm, left_hbm, depth_hbm, place_hbm,
    dec_ref, res_ref, rms_ref,
    coef, expo, right, spread, edge, keep, mix, left, depth, place,
    sbuf, rbuf, ebuf, dpad, ext, pair_out, pair_in, part, parts,
    load_sem, step_sem, send_sem, recv_sem, pair_send, pair_recv, sum_send, sum_recv,
):
    x, y, z, c = position()
    me = lax.axis_index("px") * 16 + lax.axis_index("py")
    loads = [
        pltpu.make_async_copy(src, dst, load_sem.at[n])
        for n, (src, dst) in enumerate(
            (
                (coef_hbm, coef), (expo_hbm, expo), (spread_hbm, spread), (edge_hbm, edge), (keep_hbm, keep),
                (mix_hbm, mix), (left_hbm, left), (depth_hbm, depth), (place_hbm, place), (right_hbm, right),
            )
        )
    ]
    for load in loads:
        load.start()

    entry = pltpu.get_barrier_semaphore()
    for n in range(1, 8):
        pl.semaphore_signal(entry, inc=1, device_id=ident(beside(n // 2, 0, 0, n % 2)), device_id_type=MESH)
    for n in range(1, 4):
        pl.semaphore_signal(entry, inc=1, device_id=ident(beside(0, n, 0, 0)), device_id_type=MESH)
        pl.semaphore_signal(entry, inc=1, device_id=ident(beside(0, 0, n, 0)), device_id_type=MESH)

    def clear(g, _):
        sbuf[pl.ds(g * 16, 16)] = jnp.zeros((16, ROWS, CELLS), BF16)
        return 0

    lax.fori_loop(0, 8, clear, 0)
    ebuf[0] = jnp.zeros((128, 256), F32)
    ebuf[9] = jnp.zeros((128, 256), F32)

    for load in loads[:3]:
        load.wait()

    row16 = lax.broadcasted_iota(jnp.int32, (ROWS, CELLS), 0)
    owner = lax.broadcasted_iota(jnp.int32, (ROWS, CELLS), 1) // 24

    def scale(g, _):
        base = pl.multiple_of(g * 384, 128)
        power = jnp.exp2(expo[:, pl.ds(base, 384)].astype(F32))
        rows = jnp.where(row16 < 4, power[0:1], jnp.where(row16 < 8, power[1:2], power[2:3]))
        apart = jnp.concatenate([jnp.where(owner == j, rows, 0.0) for j in range(16)], axis=0).astype(BF16)
        factor = dot(apart, spread[...])
        for j in range(16):
            at = pl.multiple_of(g * (16 * CELLS) + j * CELLS, 128)
            held = coef[:, pl.ds(at, CELLS)].astype(F32)
            sbuf[g * 16 + j, 0:LAYERS, :] = (held * factor[j * 16 : j * 16 + LAYERS]).astype(BF16)
        return 0

    lax.fori_loop(0, 8, scale, 0)

    pl.semaphore_wait(entry, 13)
    for n in range(1, 4):
        pl.semaphore_signal(step_sem.at[0], inc=1, device_id=ident(beside(0, n, 0, 0)), device_id_type=MESH)

    for load in loads[3:6]:
        load.wait()
    lane = lax.broadcasted_iota(jnp.int32, (128, 256), 1)
    even = lax.broadcasted_iota(jnp.int32, (128, 256), 0) // 8 % 2 == 0

    def edges(g, _):
        held = sbuf[pl.ds(g * 16, 16)].reshape(256, CELLS)
        wide = dot(held, edge[0]) + dot(held, edge[1])
        wide = (wide.reshape(16, ROWS, 256) * keep[...][None]).reshape(256, 256)
        hi, lo = two(wide)
        mixed = dot(mix[0], hi) + dot(mix[1], hi) + dot(mix[0], lo)
        both = jnp.where(lane < 144, mixed[:128], mixed[128:])
        ebuf[g + 1] = jnp.where(even & (lane >= 144), pltpu.roll(both, 256 - 48, 1), both)
        return 0

    lax.fori_loop(0, 8, edges, 0)

    pl.semaphore_wait(step_sem.at[0], 3)
    for n in range(1, 4):
        pl.semaphore_signal(step_sem.at[1], inc=1, device_id=ident(beside(0, 0, n, 0)), device_id_type=MESH)

    low = lane % 48 < 24
    half = lax.broadcasted_iota(jnp.int32, (128, 128), 1) < 64

    def gather(g, _):
        value = jnp.where(lane < 144, jnp.where(low, ebuf[g + 2], ebuf[g]), ebuf[g + 1])
        hi = value.astype(BF16).astype(F32)
        lo = value - hi
        first = pltpu.roll(lo[:, :128], 64, 1)
        second = pltpu.roll(lo[:, 128:], 64, 1)
        line = jnp.concatenate(
            [hi[:, :128], jnp.where(half, hi[:, 128:], first), jnp.where(half, first, second)], axis=1
        ).reshape(16, 8, CELLS)
        tall = jnp.concatenate([jnp.zeros((16, 8, CELLS), F32), line], axis=1).astype(BF16)
        sbuf[pl.ds(g * 16, 16)] = sbuf[pl.ds(g * 16, 16)] + tall
        return 0

    lax.fori_loop(0, 8, gather, 0)
    rbuf[me] = sbuf[me]
    pl.semaphore_wait(step_sem.at[1], 3)

    def message(phase, n):
        m = n * 37 % 64
        there = beside(m // 2 % 4, m // 32 * 2 + phase, m // 8 % 4, m % 2)
        return pltpu.make_async_remote_copy(
            sbuf.at[there[0] * 16 + there[1]], rbuf.at[me], send_sem, recv_sem.at[phase],
            device_id=ident(there), device_id_type=MESH,
        )

    def start(phase):
        def one(n, _):
            message(phase, n).start()
            return 0

        lax.fori_loop(1 - phase, 64, one, 0)

    start(0)
    start(1)

    for load in loads[6:]:
        load.wait()

    here = ident(beside(0, 0, 0, 1))

    def pair_copy(n, at):
        return pltpu.make_async_remote_copy(
            pair_out.at[:, pl.ds(at, 384)], pair_in.at[:, pl.ds(at, 384)], pair_send.at[n], pair_recv.at[n],
            device_id=here, device_id_type=MESH,
        )

    def decode(phase, k):
        layer = lax.rem(y + phase + 2 * k, 4)
        at = pl.multiple_of(layer * 384, 128)
        cells, sides = [], []
        for odd in range(2):
            held = rbuf[pl.ds(layer * 32 + odd * 16, 16)].reshape(256, CELLS)
            wide = dot_rows(left[...], held)
            hi, lo = two(wide[:384] + wide[384:768])
            cells.append(dot(hi, depth[odd, 0]) + dot(lo, depth[odd, 0]) + dot(hi, depth[odd, 1]))
            hi, lo = two(jnp.concatenate([wide[768:832], wide[832:896], wide[896:960]], axis=1))
            sides.append(dot(hi, place[odd]) + dot(lo, place[odd]))

        def join(pieces):
            a, b = pieces
            return jnp.concatenate([a[:, :128], a[:, 128:] + b[:, :128], b[:, 128:]], axis=1)

        field, side = join(cells), join(sides)
        dec_ref[:, pl.ds(at, 384)] = field
        dpad[24:408, pl.ds(at, 384)] = field
        dpad[0:24, pl.ds(at, 384)] = side[24:48]
        dpad[408:432, pl.ds(at, 384)] = side[0:24]
        ext[:, pl.ds(at, 384)] = side[48:64]
        cube = field.reshape(CX, CY, 384)
        pair_out[:, pl.ds(at, 384)] = jnp.where(c == 0, cube[:, 23, :], cube[:, 0, :])
        return at

    for phase in range(2):
        count = 63 + phase
        pltpu.make_async_copy(rbuf.at[pl.ds(0, count)], rbuf.at[pl.ds(0, count)], recv_sem.at[phase]).wait()
        places = [decode(phase, k) for k in range(2)]
        for k in range(2):
            pair_copy(phase * 2 + k, places[k]).start()
    for phase in range(2):
        for k in range(2):
            pair_copy(phase * 2 + k, pl.multiple_of(lax.rem(y + phase + 2 * k, 4) * 384, 128)).wait()

    column = lax.broadcasted_iota(jnp.int32, (CY, NZ), 1)
    row = lax.broadcasted_iota(jnp.int32, (CY, NZ), 0)

    def slab(n, total):
        at = pl.multiple_of(n * CY, 8)
        own = dpad[pl.ds(at + CY, CY), :]
        near = dpad[pl.ds(at, CY), :] + dpad[pl.ds(at + 2 * CY, CY), :]
        inner, outer = pair_in[pl.ds(n, 1), :], ext[pl.ds(n, 1), :]
        below = jnp.where(c == 0, outer, inner)
        above = jnp.where(c == 0, inner, outer)
        near = near + jnp.where(row == 0, below, pltpu.roll(own, 1, 0))
        near = near + jnp.where(row == CY - 1, above, pltpu.roll(own, CY - 1, 0))
        near = near + jnp.where(column == 0, 0.0, pltpu.roll(own, 1, 1))
        near = near + jnp.where(column == NZ - 1, 0.0, pltpu.roll(own, NZ - 1, 1))
        value = right[pl.ds(at, CY), :] - (6.0 * own - near)
        res_ref[pl.ds(at, CY), :] = value
        square = value * value
        square = square[0:8] + square[8:16] + square[16:24]
        return total + sum(square[:, k * 128 : (k + 1) * 128] for k in range(NZ // 128))

    total = lax.fori_loop(0, CX, slab, jnp.zeros((8, 128), F32))
    part[...] = jnp.sum(total, axis=0, keepdims=True)
    parts[me] = part[...]

    def note(n):
        m = PEERS - n
        there = beside(m // 2 % 4, m // 8 % 4, m // 32, m % 2)
        return pltpu.make_async_remote_copy(
            part, parts.at[me], sum_send, sum_recv, device_id=ident(there), device_id_type=MESH
        )

    def tell(n, _):
        note(n).start()
        return 0

    lax.fori_loop(1, PEERS, tell, 0)
    everyone = pl.ds(0, PEERS - 1)
    pltpu.make_async_copy(sbuf.at[everyone], sbuf.at[everyone], send_sem).wait()
    pltpu.make_async_copy(parts.at[everyone], parts.at[everyone], sum_send).wait()
    pltpu.make_async_copy(parts.at[everyone], parts.at[everyone], sum_recv).wait()
    whole = jnp.sum(jnp.sum(parts[...], axis=0), axis=1, keepdims=True)
    rms_ref[...] = jnp.broadcast_to(jnp.sqrt(whole / (PEERS * CELLS * NZ) + 1e-06), (8, 128))


def shards(coefficients, exponents, right_side):
    constants = tables()
    any_space = pl.BlockSpec(memory_space=pl.ANY)
    vmem = pl.BlockSpec(memory_space=pltpu.VMEM)
    right = right_side.reshape(CELLS, NZ)
    operands = (coefficients, exponents, right, *constants)
    held = [pltpu.VMEM(o.shape, o.dtype) for o in operands]
    sem = pltpu.SemaphoreType
    field = jax.ShapeDtypeStruct((CELLS, NZ), F32)
    decoded, residual, rms = pl.pallas_call(
        kernel,
        name="exchange",
        out_shape=(field, field, jax.ShapeDtypeStruct((8, 128), F32)),
        in_specs=[any_space] * len(operands),
        out_specs=(vmem, vmem, vmem),
        scratch_shapes=[
            *held,
            pltpu.VMEM((PEERS, ROWS, CELLS), BF16),
            pltpu.VMEM((PEERS, ROWS, CELLS), BF16),
            pltpu.VMEM((10, 128, 256), F32),
            pltpu.VMEM((CELLS + 2 * CY, NZ), F32),
            pltpu.VMEM((CX, NZ), F32),
            pltpu.VMEM((CX, NZ), F32),
            pltpu.VMEM((CX, NZ), F32),
            pltpu.VMEM((1, 128), F32),
            pltpu.VMEM((PEERS, 1, 128), F32),
            sem.DMA((len(operands),)),
            sem.REGULAR((2,)),
            sem.DMA,
            sem.DMA((2,)),
            sem.DMA((4,)),
            sem.DMA((4,)),
            sem.DMA,
            sem.DMA,
        ],
        compiler_params=pltpu.CompilerParams(collective_id=0, has_side_effects=True, vmem_limit_bytes=60 << 20),
    )(*operands)
    shape = (CX, CY, NZ)
    return decoded.reshape(shape), residual.reshape(shape), rms[0, 0]


def solution(mesh):
    placed = (P(("px", "py"), None), P(("px", "py"), None), P("px", "py", None))
    return jax.shard_map(
        shards,
        mesh=mesh,
        in_specs=placed,
        out_specs=(P("px", "py", None), P("px", "py", None), P()),
        check_vma=False,
    )
```

```python
import functools

import jax
import jax.numpy as jnp
import numpy as np
from jax import lax
from jax.experimental import pallas as pl
from jax.experimental.pallas import tpu as pltpu
from jax.sharding import PartitionSpec as P

CX = 16
CY = 24
CELLS = CX * CY
NZ = 1536
PEERS = 128
LAYERS = 12
ROWS = 16
F32 = jnp.float32
BF16 = jnp.bfloat16
MESH = pl.DeviceIdType.MESH
UNROLL = 2
VMEM_BYTES = 40 << 20


def basis():
    a = np.arange(4.0)[:, None]
    i = np.arange(4.0)[None, :]
    weight = np.where(a == 0, np.sqrt(0.25), np.sqrt(0.5))
    return weight * np.cos(np.pi * (2 * i + 1) * a / 8)


def halves(table):
    hi = table.astype(np.float32).astype(BF16)
    lo = (table - hi.astype(np.float64)).astype(np.float32).astype(BF16)
    return hi, lo


def block_table(width):
    b = basis()
    n = np.arange(width)
    return np.where(n[:, None] // 4 == n[None, :] // 4, b[n[:, None] % 4, n[None, :] % 4], 0.0)


def tables():
    b = basis()
    plane = np.kron(block_table(CX), block_table(CY))
    plane_hi, plane_lo = halves(plane.T)
    lane_of = np.zeros((3, 64), np.int64)
    cell_of = np.zeros(256, np.int64)
    part_of = np.full(256, -1)
    for k in range(3):
        for e in range(64):
            lane_of[k, e] = k * 48 + e if e < 48 else 144 + k * 16 + e - 48
        for e in range(24):
            cell_of[k * 48 + e] = e
            cell_of[k * 48 + 24 + e] = 15 * CY + e
        for x in range(16):
            cell_of[144 + k * 16 + x] = x * CY
            cell_of[192 + k * 16 + x] = x * CY + 23
        for first, size in ((k * 48, 48), (144 + k * 16, 16), (192 + k * 16, 16)):
            part_of[first : first + size] = k
    edge = np.where(part_of[None, :] >= 0, plane[:, cell_of], 0.0)
    edge_hi, edge_lo = halves(edge)
    part = np.broadcast_to(part_of[None, :], (8, 256)).astype(np.int32)
    turn = np.zeros((4, 8, 128), np.float32)
    for s in range(4):
        for r in range(4, 8):
            turn[s, r, :] = b[(r + s) % 4, r % 4]
    pick = np.zeros((192, 256))
    for k in range(3):
        for e in range(64):
            pick[k * 64 + e, lane_of[k, e]] = 1
    pick_hi = pick.astype(BF16)
    pick_lo = np.roll(pick, 64, axis=1).astype(BF16)
    left = np.stack(
        [
            np.concatenate([plane_hi[:192, :256], plane_lo[:192, :256], pick_hi]),
            np.concatenate([plane_hi[192:, 128:], plane_lo[192:, 128:], pick_lo]),
        ]
    )
    depth = np.zeros((2, 256, 256))
    place = np.zeros((2, 768, 256))
    for odd in range(2):
        for s in range(16):
            base = 64 * odd + s * LAYERS
            for z in range(LAYERS):
                for o in range(z // 4 * 4, z // 4 * 4 + 4):
                    depth[odd, s * 16 + z, base + o] = b[z % 4, o % 4]
            for k in range(3):
                for r in range(4):
                    place[odd, k * 256 + s * 16 + 12 + r, base + k * 4 + r] = 1
    depth_hi, depth_lo = halves(depth)
    column = np.arange(CELLS)
    spread = (column[:, None] % 24 == (column[None, :] // CY // 4) * 6 + column[None, :] % CY // 4).astype(BF16)
    return (
        spread,
        np.concatenate([edge_hi, edge_lo], axis=1),
        part,
        turn,
        left,
        np.stack([depth_hi, depth_lo], axis=1),
        place.astype(BF16),
    )


def dot(a, b):
    return lax.dot_general(a, b, (((1,), (0,)), ((), ())), preferred_element_type=F32)


def dot_rows(a, b):
    return lax.dot_general(a, b, (((1,), (1,)), ((), ())), preferred_element_type=F32)


def two(x):
    hi = x.astype(BF16)
    return hi, (x - hi.astype(F32)).astype(BF16)


def position():
    i, j = lax.axis_index("px"), lax.axis_index("py")
    return ((j >> 1) & 1) * 2 + (i & 1), i >> 1, j >> 2, j & 1


class Peers:
    def __init__(self):
        x, y, z, c = position()
        xs = [(x + d) & 3 for d in range(4)]
        self.x_low = [v & 1 for v in xs]
        self.x_high = [v & 2 for v in xs]
        self.y_part = [((y + d) & 3) * 2 for d in range(4)]
        self.z = z
        self.y = y
        self.core = [c, 1 - c]

    def z_part(self, d):
        return ((self.z + d) & 3) * 4

    def at(self, dx, dy, dz, dc):
        y = self.y_part[dy] if isinstance(dy, int) else ((self.y + dy) & 3) * 2
        return y + self.x_low[dx], self.z_part(dz) + self.x_high[dx] + self.core[dc]


def ident(pair):
    return {"px": pair[0], "py": pair[1]}


def kernel(
    coef_hbm, expo_hbm, right_hbm, spread_hbm, edge_hbm, part_hbm, turn_hbm, left_hbm, depth_hbm, place_hbm,
    dec_ref, res_ref, rms_ref,
    coef, expo, right, spread, edge, part_of, turn, left, depth, place,
    sbuf, rbuf, ebuf, dpad, ext, pair_out, pair_in, part, parts,
    load_sem, step_sem, send_sem, recv_sem, pair_send, pair_recv, sum_send, sum_recv,
):
    x, y, z, c = position()
    peers = Peers()
    me = lax.axis_index("px") * 16 + lax.axis_index("py")
    loads = [
        pltpu.make_async_copy(src, dst, load_sem.at[n])
        for n, (src, dst) in enumerate(
            (
                (coef_hbm, coef), (expo_hbm, expo), (spread_hbm, spread), (edge_hbm, edge), (part_hbm, part_of),
                (turn_hbm, turn), (left_hbm, left), (depth_hbm, depth), (place_hbm, place), (right_hbm, right),
            )
        )
    ]
    for load in loads:
        load.start()

    entry = pltpu.get_barrier_semaphore()
    for n in range(1, 8):
        pl.semaphore_signal(entry, inc=1, device_id=ident(peers.at(n // 2, 0, 0, n % 2)), device_id_type=MESH)
    for n in range(1, 4):
        pl.semaphore_signal(entry, inc=1, device_id=ident(peers.at(0, n, 0, 0)), device_id_type=MESH)
        pl.semaphore_signal(entry, inc=1, device_id=ident(peers.at(0, 0, n, 0)), device_id_type=MESH)

    def clear(g, _):
        sbuf[pl.ds(g * 16, 16), 8:16, :] = jnp.zeros((16, 8, CELLS), BF16)
        ebuf[g + 1, 0] = jnp.zeros((8, 256), F32)
        ebuf[g + 1, 17] = jnp.zeros((8, 256), F32)
        return 0

    lax.fori_loop(0, 8, clear, 0)
    ebuf[0] = jnp.zeros((18, 8, 256), F32)
    ebuf[9] = jnp.zeros((18, 8, 256), F32)

    with jax.named_scope("s_load"):
        for load in loads[:6]:
            load.wait()

    row16 = lax.broadcasted_iota(jnp.int32, (ROWS, CELLS), 0)
    owner = lax.broadcasted_iota(jnp.int32, (ROWS, CELLS), 1) // 24
    upper = lax.broadcasted_iota(jnp.int32, (16, 8, 256), 1) < 4

    def scale(g, _):
        base = pl.multiple_of(g * 384, 128)
        power = jnp.exp2(expo[:, pl.ds(base, 384)].astype(F32))
        rows = jnp.where(row16 < 4, power[0:1], jnp.where(row16 < 8, power[1:2], power[2:3]))
        apart = jnp.concatenate([jnp.where(owner == j, rows, 0.0) for j in range(16)], axis=0).astype(BF16)
        factor = dot(apart, spread[...])
        for j in range(16):
            at = pl.multiple_of(g * (16 * CELLS) + j * CELLS, 128)
            held = coef[:, pl.ds(at, CELLS)].astype(F32)
            sbuf[g * 16 + j, 0:LAYERS, :] = (held * factor[j * 16 : j * 16 + LAYERS]).astype(BF16)
        return 0

    def edges(g, _):
        held = sbuf[pl.ds(g * 16, 16)].reshape(256, CELLS)
        wide = dot(held, edge[...])
        wide = (wide[:, :256] + wide[:, 256:]).reshape(16, ROWS, 256)
        first, second = wide[:, :8], wide[:, 8:]
        first_turned, second_turned = pltpu.roll(first, 4, 1), pltpu.roll(second, 4, 1)
        kind = part_of[...][None]
        four = jnp.where(
            kind == 0,
            jnp.where(upper, first, first_turned),
            jnp.where(
                kind == 1, jnp.where(upper, first_turned, first), jnp.where(upper, second, second_turned)
            ),
        )
        weights = [jnp.concatenate([turn[s], turn[s]], axis=1)[None] for s in range(4)]
        mixed = four * weights[0]
        for s in range(1, 4):
            mixed = mixed + pltpu.roll(four, 8 - s, 1) * weights[s]
        ebuf[g + 1, 1:17] = mixed
        return 0

    with jax.named_scope("s_scale"):
        lax.fori_loop(0, 8, scale, 0, unroll=UNROLL)

    with jax.named_scope("s_bar1"):
        pl.semaphore_wait(entry, 13)
    for n in range(1, 4):
        pl.semaphore_signal(step_sem.at[0], inc=1, device_id=ident(peers.at(0, n, 0, 0)), device_id_type=MESH)

    with jax.named_scope("s_edges"):
        lax.fori_loop(0, 8, edges, 0, unroll=UNROLL)

    with jax.named_scope("s_bar2"):
        pl.semaphore_wait(step_sem.at[0], 3)
    for n in range(1, 4):
        pl.semaphore_signal(step_sem.at[1], inc=1, device_id=ident(peers.at(0, 0, n, 0)), device_id_type=MESH)

    lane = lax.broadcasted_iota(jnp.int32, (16, 8, 256), 2)
    low = lane % 48 < 24
    across = lane < 144
    half = lax.broadcasted_iota(jnp.int32, (16, 8, 128), 2) < 64
    even = lax.broadcasted_iota(jnp.int32, (16, 8, 128), 0) % 2 == 0

    def gather(g, _):
        value = jnp.where(low, ebuf[g + 2, 1:17], ebuf[g, 1:17])
        along = jnp.where(even, pltpu.roll(ebuf[g + 1, 0:16, :, 128:], 80, 2), ebuf[g + 1, 2:18, :, 128:])
        one = value[:, :, :128]
        two_ = jnp.where(across[:, :, 128:], value[:, :, 128:], along)
        one_hi = one.astype(BF16).astype(F32)
        two_hi = two_.astype(BF16).astype(F32)
        first = pltpu.roll(one - one_hi, 64, 2)
        second = pltpu.roll(two_ - two_hi, 64, 2)
        line = jnp.concatenate([one_hi, jnp.where(half, two_hi, first), jnp.where(half, first, second)], axis=2)
        tall = jnp.concatenate([jnp.zeros((16, 8, CELLS), F32), line], axis=1).astype(BF16)
        sbuf[pl.ds(g * 16, 16)] = sbuf[pl.ds(g * 16, 16)] + tall
        return 0

    with jax.named_scope("s_gather"):
        lax.fori_loop(0, 8, gather, 0)
    rbuf[me] = sbuf[me]
    with jax.named_scope("s_bar3"):
        pl.semaphore_wait(step_sem.at[1], 3)

    def start(phase):
        def one(i, _):
            for j in range(8):
                def go(j=j):
                    there = peers.at((j & 1) * 2 + phase % 2, (j >> 1 & 1) * 2 + phase // 2, i + j, j >> 2)
                    pltpu.make_async_remote_copy(
                        sbuf.at[there[0] * 16 + there[1]], rbuf.at[me], send_sem, recv_sem.at[phase],
                        device_id=ident(there), device_id_type=MESH,
                    ).start()

                if phase == 0 and j == 0:
                    pl.when(i > 0)(go)
                else:
                    go()
            return 0

        lax.fori_loop(0, 4, one, 0)

    with jax.named_scope("s_start"):
        for phase in range(4):
            start(phase)

    for load in loads[6:]:
        load.wait()

    def wipe(n, _):
        dpad[n] = jnp.zeros((CY, NZ + 256), F32)
        return 0

    lax.fori_loop(0, CX + 2, wipe, 0)
    ext[...] = jnp.zeros((CX, NZ), F32)

    here = ident(peers.at(0, 0, 0, 1))

    def layer(parity, k):
        return (y + parity + 2 * k) & 3

    def pair_copy(parity, k):
        at = pl.multiple_of(layer(parity, k) * 384, 128)
        n = parity * 2 + k
        return pltpu.make_async_remote_copy(
            pair_out.at[:, pl.ds(at, 384)], pair_in.at[:, pl.ds(at, 384)], pair_send.at[n], pair_recv.at[n],
            device_id=here, device_id_type=MESH,
        )

    def pair_start(parity, k):
        at = layer(parity, k) * 384
        lanes = pl.ds(pl.multiple_of(at + 128, 128), 384)
        last = dpad[1 : CX + 1, CY - 8 :, lanes][:, 7, :]
        first = dpad[1 : CX + 1, 0:8, lanes][:, 0, :]
        pair_out[:, pl.ds(pl.multiple_of(at, 128), 384)] = jnp.where(c == 0, last, first)
        pair_copy(parity, k).start()

    def decode(phase, k):
        odd = (x + phase) & 1
        group = layer(phase // 2, k) * 2 + odd
        at = layer(phase // 2, k) * 384 + odd * 128
        held = rbuf[pl.ds(group * 16, 16)].reshape(256, CELLS)
        near = dot_rows(left[0], held[:, :256])
        far = dot_rows(left[1], held[:, 128:])
        hi, lo = two(jnp.concatenate([near[:192] + near[192:384], far[:192] + far[192:384]], axis=0))
        table = depth[odd, 0]
        field = dot(hi, table) + dot(lo, table) + dot(hi, depth[odd, 1])
        side_hi = jnp.concatenate([near[384:448], near[448:512], near[512:576]], axis=1).astype(BF16)
        side_lo = jnp.concatenate([far[384:448], far[448:512], far[512:576]], axis=1).astype(BF16)
        table = place[odd]
        side = dot(side_hi, table) + dot(side_lo, table)
        lanes = pl.ds(pl.multiple_of(at + 128, 128), 256)
        dpad[1 : CX + 1, :, lanes] += field.reshape(CX, CY, 256)
        dpad[0, :, lanes] += side[24:48]
        dpad[CX + 1, :, lanes] += side[0:24]
        ext[:, pl.ds(pl.multiple_of(at, 128), 256)] += side[48:64]

    column = lax.broadcasted_iota(jnp.int32, (CY, 384), 1)
    row = lax.broadcasted_iota(jnp.int32, (CY, 384), 0)
    tile = lax.broadcasted_iota(jnp.int32, (CY, 128), 1)

    def squares(value):
        value = value * value
        value = value[0:8] + value[8:16] + value[16:24]
        return sum(value[:, k * 128 : (k + 1) * 128] for k in range(value.shape[1] // 128))

    def residual(parity, k, total):
        at = layer(parity, k) * 384
        lanes = pl.ds(pl.multiple_of(at, 128), 384)
        inside = pl.ds(pl.multiple_of(at + 128, 128), 384)

        def slab(n, total):
            rows = pl.multiple_of(n * CY, 8)
            own = dpad[n + 1, :, inside]
            near = dpad[n, :, inside] + dpad[n + 2, :, inside]
            inner, outer = pair_in[pl.ds(n, 1), lanes], ext[pl.ds(n, 1), lanes]
            below = jnp.where(c == 0, outer, inner)
            above = jnp.where(c == 0, inner, outer)
            near = near + jnp.where(row == 0, below, pltpu.roll(own, 1, 0))
            near = near + jnp.where(row == CY - 1, above, pltpu.roll(own, CY - 1, 0))
            back, forth = pltpu.roll(own, 1, 1), pltpu.roll(own, 383, 1)
            if parity == 0:
                back = jnp.where(column == 0, 0.0, back)
                forth = jnp.where(column == 383, 0.0, forth)
            else:
                prior = dpad[n + 1, :, pl.ds(pl.multiple_of(at, 128), 128)]
                later = dpad[n + 1, :, pl.ds(pl.multiple_of(at + 512, 128), 128)]
                back = jnp.concatenate(
                    [jnp.where(tile == 0, pltpu.roll(prior, 1, 1), back[:, :128]), back[:, 128:]], axis=1
                )
                forth = jnp.concatenate(
                    [forth[:, :256], jnp.where(tile == 127, pltpu.roll(later, 127, 1), forth[:, 256:])], axis=1
                )
            value = right[pl.ds(rows, CY), lanes] - (6.0 * own - (near + back + forth))
            dec_ref[pl.ds(rows, CY), lanes] = own
            res_ref[pl.ds(rows, CY), lanes] = value
            if parity == 0:
                value = jnp.where((column > 0) & (column < 383), value, 0.0)
            return total + squares(value)

        return lax.fori_loop(0, CX, slab, total, unroll=4)

    def seam(k, total):
        at = layer(0, k) * 384

        def slab(n, total):
            rows = pl.multiple_of(n * CY, 8)
            out = pl.ds(rows, CY)
            front = pl.ds(pl.multiple_of(at, 128), 128)
            prior = pltpu.roll(dpad[n + 1, :, front], 1, 1)
            value = res_ref[out, front] + jnp.where(tile == 0, prior, 0.0)
            res_ref[out, front] = value
            total = total + squares(jnp.where(tile == 0, value, 0.0))
            back = pl.ds(pl.multiple_of(at + 256, 128), 128)
            later = pltpu.roll(dpad[n + 1, :, pl.ds(pl.multiple_of(at + 512, 128), 128)], 127, 1)
            value = res_ref[out, back] + jnp.where(tile == 127, later, 0.0)
            res_ref[out, back] = value
            return total + squares(jnp.where(tile == 127, value, 0.0))

        return lax.fori_loop(0, CX, slab, total, unroll=4)

    total = jnp.zeros((8, 128), F32)
    for phase in range(4):
        count = 32 - (phase == 0)
        block = rbuf.at[pl.ds(0, count)]
        with jax.named_scope("s_wait"):
            pltpu.make_async_copy(block, block, recv_sem.at[phase]).wait()
        with jax.named_scope("s_decode"):
            for k in range(2):
                decode(phase, k)
                if phase % 2 == 1:
                    pair_start(phase // 2, k)
        if phase == 2:
            with jax.named_scope("s_early"):
                for k in range(2):
                    pair_copy(0, k).wait()
                    total = residual(0, k, total)
    with jax.named_scope("s_seam"):
        for k in range(2):
            total = seam(k, total)
    with jax.named_scope("s_pair"):
        for k in range(2):
            pair_copy(1, k).wait()
    with jax.named_scope("s_late"):
        for k in range(2):
            total = residual(1, k, total)

    part[...] = jnp.sum(total, axis=0, keepdims=True)
    parts[me] = part[...]

    def tell(i, _):
        for j in range(8):
            def go(j=j):
                there = peers.at((2, 1, 3, 0)[j >> 1], i + 2, (i >> 2) + 2, 1 - (j & 1))
                pltpu.make_async_remote_copy(
                    part, parts.at[me], sum_send, sum_recv, device_id=ident(there), device_id_type=MESH
                ).start()

            if j == 7:
                pl.when(i != 10)(go)
            else:
                go()
        return 0

    with jax.named_scope("s_tell"):
        lax.fori_loop(0, 16, tell, 0)
    everyone = pl.ds(0, PEERS - 1)
    with jax.named_scope("s_sent"):
        pltpu.make_async_copy(sbuf.at[everyone], sbuf.at[everyone], send_sem).wait()
    with jax.named_scope("s_sum"):
        pltpu.make_async_copy(parts.at[everyone], parts.at[everyone], sum_recv).wait()
    pltpu.make_async_copy(parts.at[everyone], parts.at[everyone], sum_send).wait()
    whole = jnp.sum(jnp.sum(parts[...], axis=0), axis=1, keepdims=True)
    rms_ref[0, 0] = jnp.sqrt(whole / (PEERS * CELLS * NZ) + 1e-06)[0, 0]


def deliver(dec_ref, res_ref, dec_out, res_out, sems):
    copies = [
        pltpu.make_async_copy(src, dst, sems.at[n])
        for n, (src, dst) in enumerate(((dec_ref, dec_out), (res_ref, res_out)))
    ]
    for copy in copies:
        copy.start()
    for copy in copies:
        copy.wait()


def shards(coefficients, exponents, right_side):
    constants = tables()
    any_space = pl.BlockSpec(memory_space=pltpu.HBM)
    vmem = pl.BlockSpec(memory_space=pltpu.VMEM)
    right = right_side.reshape(CELLS, NZ)
    operands = (coefficients, exponents, right, *constants)
    operands = tuple(pltpu.with_memory_space_constraint(jnp.asarray(o), pltpu.HBM) for o in operands)
    held = [pltpu.VMEM(o.shape, o.dtype) for o in operands]
    sem = pltpu.SemaphoreType
    field = jax.ShapeDtypeStruct((CELLS, NZ), F32)
    decoded, residual, rms = pl.pallas_call(
        kernel,
        name="exchange",
        out_shape=(field, field, jax.ShapeDtypeStruct((1, 1), F32)),
        in_specs=[any_space] * len(operands),
        out_specs=(vmem, vmem, pl.BlockSpec(memory_space=pltpu.SMEM)),
        scratch_shapes=[
            *held,
            pltpu.VMEM((PEERS, ROWS, CELLS), BF16),
            pltpu.VMEM((PEERS, ROWS, CELLS), BF16),
            pltpu.VMEM((10, 18, 8, 256), F32),
            pltpu.VMEM((CX + 2, CY, NZ + 256), F32),
            pltpu.VMEM((CX, NZ), F32),
            pltpu.VMEM((CX, NZ), F32),
            pltpu.VMEM((CX, NZ), F32),
            pltpu.VMEM((1, 128), F32),
            pltpu.VMEM((PEERS, 1, 128), F32),
            sem.DMA((len(operands),)),
            sem.REGULAR((2,)),
            sem.DMA,
            sem.DMA((4,)),
            sem.DMA((4,)),
            sem.DMA((4,)),
            sem.DMA,
            sem.DMA,
        ],
        compiler_params=pltpu.CompilerParams(collective_id=0, has_side_effects=True, vmem_limit_bytes=VMEM_BYTES),
    )(*operands)
    shape = (CX, CY, NZ)
    decoded, residual = pl.pallas_call(
        deliver,
        name="deliver",
        out_shape=(field, field),
        in_specs=(vmem, vmem),
        out_specs=(any_space, any_space),
        scratch_shapes=[sem.DMA((2,))],
        compiler_params=pltpu.CompilerParams(vmem_limit_bytes=1 << 20),
    )(decoded, residual)
    return decoded.reshape(shape), residual.reshape(shape), rms[0, 0]


def solution(mesh):
    placed = (P(("px", "py"), None), P(("px", "py"), None), P("px", "py", None))
    return jax.shard_map(
        shards,
        mesh=mesh,
        in_specs=placed,
        out_specs=(P("px", "py", None), P("px", "py", None), P()),
        check_vma=False,
    )
```

```python
import random

import jax
import jax.numpy as jnp
import numpy as np
from jax import lax
from jax.experimental import pallas as pl
from jax.experimental.pallas import tpu as pltpu
from jax.sharding import PartitionSpec as P

CX = 16
CY = 24
CELLS = CX * CY
NZ = 1536
PEERS = 128
LAYERS = 12
CHUNK = CELLS * PEERS // 4
ROWS = 16
F32 = jnp.float32
BF16 = jnp.bfloat16
MESH = pl.DeviceIdType.MESH
VMEM_BYTES = 40 << 20


def basis():
    a = np.arange(4.0)[:, None]
    i = np.arange(4.0)[None, :]
    weight = np.where(a == 0, np.sqrt(0.25), np.sqrt(0.5))
    return weight * np.cos(np.pi * (2 * i + 1) * a / 8)


def halves(table):
    hi = table.astype(np.float32).astype(BF16)
    lo = (table - hi.astype(np.float64)).astype(np.float32).astype(BF16)
    return hi, lo


def block_table(width):
    b = basis()
    n = np.arange(width)
    return np.where(n[:, None] // 4 == n[None, :] // 4, b[n[:, None] % 4, n[None, :] % 4], 0.0)


def tables():
    b = basis()
    plane = np.kron(block_table(CX), block_table(CY))
    plane_hi, plane_lo = halves(plane.T)
    lane_of = np.zeros((3, 64), np.int64)
    cell_of = np.zeros(256, np.int64)
    part_of = np.full(256, -1)
    for k in range(3):
        for e in range(64):
            lane_of[k, e] = k * 48 + e if e < 48 else 144 + k * 16 + e - 48
        for e in range(24):
            cell_of[k * 48 + e] = e
            cell_of[k * 48 + 24 + e] = 15 * CY + e
        for x in range(16):
            cell_of[144 + k * 16 + x] = x * CY
            cell_of[192 + k * 16 + x] = x * CY + 23
        for first, size in ((k * 48, 48), (144 + k * 16, 16), (192 + k * 16, 16)):
            part_of[first : first + size] = k
    edge = np.where(part_of[None, :] >= 0, plane[:, cell_of], 0.0)
    edge_hi, edge_lo = halves(edge)
    part = np.broadcast_to(part_of[None, :], (8, 256)).astype(np.int32)
    turn = np.zeros((4, 8, 128), np.float32)
    for s in range(4):
        for r in range(4, 8):
            turn[s, r, :] = b[(r + s) % 4, r % 4]
    pick = np.zeros((192, 256))
    for k in range(3):
        for e in range(64):
            pick[k * 64 + e, lane_of[k, e]] = 1
    pick_hi = pick.astype(BF16)
    pick_lo = np.roll(pick, 64, axis=1).astype(BF16)
    left = np.stack(
        [
            np.concatenate([plane_hi[:192, :256], plane_lo[:192, :256], pick_hi]),
            np.concatenate([plane_hi[192:, 128:], plane_lo[192:, 128:], pick_lo]),
        ]
    )
    depth = np.zeros((2, 256, 256))
    place = np.zeros((2, 768, 256))
    for odd in range(2):
        for s in range(16):
            base = 64 * odd + s * LAYERS
            for z in range(LAYERS):
                for o in range(z // 4 * 4, z // 4 * 4 + 4):
                    depth[odd, s * 16 + z, base + o] = b[z % 4, o % 4]
            for k in range(3):
                for r in range(4):
                    place[odd, k * 256 + s * 16 + 12 + r, base + k * 4 + r] = 1
    depth_hi, depth_lo = halves(depth)
    column = np.arange(CELLS)
    spread = (column[:, None] % 24 == (column[None, :] // CY // 4) * 6 + column[None, :] % CY // 4).astype(BF16)
    return (
        spread,
        np.concatenate([edge_hi, edge_lo], axis=1),
        part,
        turn,
        left,
        np.stack([depth_hi, depth_lo], axis=1),
        place.astype(BF16),
    )


def dot(a, b):
    return lax.dot_general(a, b, (((1,), (0,)), ((), ())), preferred_element_type=F32)


def dot_rows(a, b):
    return lax.dot_general(a, b, (((1,), (1,)), ((), ())), preferred_element_type=F32)


def two(x):
    hi = x.astype(BF16)
    return hi, (x - hi.astype(F32)).astype(BF16)


def position():
    i, j = lax.axis_index("px"), lax.axis_index("py")
    return ((j >> 1) & 1) * 2 + (i & 1), i >> 1, j >> 2, j & 1


def orders():
    every = [(i, j, k, m) for k in range(4) for j in range(4) for i in range(4) for m in range(2)]
    every = every[1:] if every[0] == (0, 0, 0, 0) else every
    random.Random(0).shuffle(every)
    return [[d for d in every if d[0] % 2 == phase % 2 and d[1] % 2 == phase // 2] for phase in range(4)]


class Peers:
    def __init__(self):
        x, y, z, c = position()
        xs = [(x + d) & 3 for d in range(4)]
        self.x_low = [v & 1 for v in xs]
        self.x_high = [v & 2 for v in xs]
        self.y_part = [((y + d) & 3) * 2 for d in range(4)]
        self.z = z
        self.y = y
        self.core = [c, 1 - c]

    def z_part(self, d):
        return ((self.z + d) & 3) * 4

    def at(self, dx, dy, dz, dc):
        y = self.y_part[dy] if isinstance(dy, int) else ((self.y + dy) & 3) * 2
        return y + self.x_low[dx], self.z_part(dz) + self.x_high[dx] + self.core[dc]


def ident(pair):
    return {"px": pair[0], "py": pair[1]}


def kernel(
    coef_hbm, expo_hbm, right_hbm, spread_hbm, edge_hbm, part_hbm, turn_hbm, left_hbm, depth_hbm, place_hbm,
    dec_ref, res_ref, rms_ref,
    coef, expo, right, spread, edge, part_of, turn, left, depth, place,
    sbuf, rbuf, ebuf, dpad, ext, pair_out, pair_in, part, parts,
    load_sem, send_sem, recv_sem, pair_send, pair_recv, sum_send, sum_recv,
):
    x, y, z, c = position()
    peers = Peers()
    me = lax.axis_index("px") * 16 + lax.axis_index("py")
    def load(n, src, dst):
        return pltpu.make_async_copy(src, dst, load_sem.at[n])

    chunks = [
        load(n, coef_hbm.at[:, pl.ds(n * CHUNK, CHUNK)], coef.at[:, pl.ds(n * CHUNK, CHUNK)])
        for n in range(4)
    ]
    first = [load(4, expo_hbm, expo), load(5, spread_hbm, spread)]
    second = [load(6, edge_hbm, edge), load(7, part_hbm, part_of), load(8, turn_hbm, turn)]
    third = [load(9, left_hbm, left), load(10, depth_hbm, depth), load(11, place_hbm, place)]
    third.append(load(12, right_hbm, right))
    for copy in [*first, *chunks, *second]:
        copy.start()

    entry = pltpu.get_barrier_semaphore()
    def everywhere(act):
        def one(i, _):
            for j in range(8):
                def go(j=j):
                    act(ident(peers.at((2, 1, 3, 0)[j >> 1], i + 2, (i >> 2) + 2, 1 - (j & 1))))

                if j == 7:
                    pl.when(i != 10)(go)
                else:
                    go()
            return 0

        lax.fori_loop(0, 16, one, 0)

    with jax.named_scope("s_signal"):
        everywhere(lambda there: pl.semaphore_signal(entry, inc=1, device_id=there, device_id_type=MESH))

    def clear(g, _):
        sbuf[pl.ds(g * 16, 16), 8:16, :] = jnp.zeros((16, 8, CELLS), BF16)
        ebuf[g + 1, 0] = jnp.zeros((8, 256), F32)
        ebuf[g + 1, 17] = jnp.zeros((8, 256), F32)
        return 0

    lax.fori_loop(0, 8, clear, 0)
    ebuf[0] = jnp.zeros((18, 8, 256), F32)
    ebuf[9] = jnp.zeros((18, 8, 256), F32)

    with jax.named_scope("s_load"):
        for copy in first:
            copy.wait()

    row16 = lax.broadcasted_iota(jnp.int32, (ROWS, CELLS), 0)
    owner = lax.broadcasted_iota(jnp.int32, (ROWS, CELLS), 1) // 24
    upper = lax.broadcasted_iota(jnp.int32, (16, 8, 256), 1) < 4

    def scale(h):
        apart = []
        for g in (2 * h, 2 * h + 1):
            power = jnp.exp2(expo[:, g * 384 : g * 384 + 384].astype(F32))
            rows = jnp.where(row16 < 4, power[0:1], jnp.where(row16 < 8, power[1:2], power[2:3]))
            apart += [jnp.where(owner == j, rows, 0.0) for j in range(16)]
        factor = dot(jnp.concatenate(apart, axis=0).astype(BF16), spread[...])
        for j in range(32):
            at = (h * 32 + j) * CELLS
            held = coef[:, at : at + CELLS].astype(F32)
            sbuf[h * 32 + j, 0:LAYERS, :] = (held * factor[j * 16 : j * 16 + LAYERS]).astype(BF16)

    def edges(h):
        held = sbuf[h * 32 : h * 32 + 32].reshape(512, CELLS)
        both = dot(held, edge[...])
        both = (both[:, :256] + both[:, 256:]).reshape(32, ROWS, 256)
        kind = part_of[...][None]
        weights = [jnp.concatenate([turn[s], turn[s]], axis=1)[None] for s in range(4)]
        for n in range(2):
            wide = both[n * 16 : n * 16 + 16]
            first, second = wide[:, :8], wide[:, 8:]
            first_turned, second_turned = pltpu.roll(first, 4, 1), pltpu.roll(second, 4, 1)
            four = jnp.where(
                kind == 0,
                jnp.where(upper, first, first_turned),
                jnp.where(
                    kind == 1, jnp.where(upper, first_turned, first), jnp.where(upper, second, second_turned)
                ),
            )
            mixed = four * weights[0]
            for s in range(1, 4):
                mixed = mixed + pltpu.roll(four, 8 - s, 1) * weights[s]
            ebuf[h * 2 + n + 1, 1:17] = mixed

    with jax.named_scope("s_scale"):
        for h in range(4):
            chunks[h].wait()
            scale(h)

    for copy in third:
        copy.start()
    for copy in second:
        copy.wait()

    with jax.named_scope("s_edges"):
        for h in range(4):
            edges(h)

    lane = lax.broadcasted_iota(jnp.int32, (16, 8, 256), 2)
    low = lane % 48 < 24
    across = lane < 144
    half = lax.broadcasted_iota(jnp.int32, (16, 8, 128), 2) < 64
    even = lax.broadcasted_iota(jnp.int32, (16, 8, 128), 0) % 2 == 0

    def layer(parity, k):
        return (y + parity + 2 * k) & 3

    def gather(g):
        value = jnp.where(low, ebuf[g + 2, 1:17], ebuf[g, 1:17])
        along = jnp.where(even, pltpu.roll(ebuf[g + 1, 0:16, :, 128:], 80, 2), ebuf[g + 1, 2:18, :, 128:])
        one = value[:, :, :128]
        two_ = jnp.where(across[:, :, 128:], value[:, :, 128:], along)
        one_hi = one.astype(BF16).astype(F32)
        two_hi = two_.astype(BF16).astype(F32)
        first = pltpu.roll(one - one_hi, 64, 2)
        second = pltpu.roll(two_ - two_hi, 64, 2)
        line = jnp.concatenate([one_hi, jnp.where(half, two_hi, first), jnp.where(half, first, second)], axis=2)
        tall = jnp.concatenate([jnp.zeros((16, 8, CELLS), F32), line], axis=1).astype(BF16)
        sbuf[pl.ds(g * 16, 16)] = sbuf[pl.ds(g * 16, 16)] + tall

    def collect(phase):
        for k in range(2):
            gather(layer(phase // 2, k) * 2 + ((x + phase) & 1))

    def start(phase):
        for distance in orders()[phase]:
            there = peers.at(*distance)
            pltpu.make_async_remote_copy(
                sbuf.at[there[0] * 16 + there[1]], rbuf.at[me], send_sem, recv_sem.at[phase],
                device_id=ident(there), device_id_type=MESH,
            ).start()

    with jax.named_scope("s_gather"):
        collect(0)
        collect(1)
    with jax.named_scope("s_bar"):
        pl.semaphore_wait(entry, PEERS - 1)
    with jax.named_scope("s_start"):
        start(0)
        collect(2)
        start(1)
        collect(3)
        start(2)
        rbuf[me] = sbuf[me]
        start(3)

    for copy in third:
        copy.wait()

    def wipe(n, _):
        dpad[n] = jnp.zeros((CY, NZ + 256), F32)
        return 0

    lax.fori_loop(0, CX + 2, wipe, 0)
    ext[...] = jnp.zeros((CX, NZ), F32)

    here = ident(peers.at(0, 0, 0, 1))

    def pair_copy(parity, k):
        at = pl.multiple_of(layer(parity, k) * 384, 128)
        n = parity * 2 + k
        return pltpu.make_async_remote_copy(
            pair_out.at[:, pl.ds(at, 384)], pair_in.at[:, pl.ds(at, 384)], pair_send.at[n], pair_recv.at[n],
            device_id=here, device_id_type=MESH,
        )

    def pair_start(parity, k):
        at = layer(parity, k) * 384
        lanes = pl.ds(pl.multiple_of(at + 128, 128), 384)
        last = dpad[1 : CX + 1, CY - 8 :, lanes][:, 7, :]
        first = dpad[1 : CX + 1, 0:8, lanes][:, 0, :]
        pair_out[:, pl.ds(pl.multiple_of(at, 128), 384)] = jnp.where(c == 0, last, first)
        pair_copy(parity, k).start()

    def decode(phase, k):
        odd = (x + phase) & 1
        group = layer(phase // 2, k) * 2 + odd
        at = layer(phase // 2, k) * 384 + odd * 128
        held = rbuf[pl.ds(group * 16, 16)].reshape(256, CELLS)
        near = dot_rows(left[0], held[:, :256])
        far = dot_rows(left[1], held[:, 128:])
        hi, lo = two(jnp.concatenate([near[:192] + near[192:384], far[:192] + far[192:384]], axis=0))
        table = depth[odd, 0]
        field = dot(hi, table) + dot(lo, table) + dot(hi, depth[odd, 1])
        side_hi = jnp.concatenate([near[384:448], near[448:512], near[512:576]], axis=1).astype(BF16)
        side_lo = jnp.concatenate([far[384:448], far[448:512], far[512:576]], axis=1).astype(BF16)
        table = place[odd]
        side = dot(side_hi, table) + dot(side_lo, table)
        lanes = pl.ds(pl.multiple_of(at + 128, 128), 256)
        dpad[1 : CX + 1, :, lanes] += field.reshape(CX, CY, 256)
        dpad[0, :, lanes] += side[24:48]
        dpad[CX + 1, :, lanes] += side[0:24]
        ext[:, pl.ds(pl.multiple_of(at, 128), 256)] += side[48:64]

    column = lax.broadcasted_iota(jnp.int32, (CY, 384), 1)
    row = lax.broadcasted_iota(jnp.int32, (CY, 384), 0)
    tile = lax.broadcasted_iota(jnp.int32, (CY, 128), 1)

    def squares(value):
        value = value * value
        value = value[0:8] + value[8:16] + value[16:24]
        return sum(value[:, k * 128 : (k + 1) * 128] for k in range(value.shape[1] // 128))

    def residual(parity, k, total):
        at = layer(parity, k) * 384
        lanes = pl.ds(pl.multiple_of(at, 128), 384)
        inside = pl.ds(pl.multiple_of(at + 128, 128), 384)

        def slab(n, total):
            rows = pl.multiple_of(n * CY, 8)
            own = dpad[n + 1, :, inside]
            near = dpad[n, :, inside] + dpad[n + 2, :, inside]
            inner, outer = pair_in[pl.ds(n, 1), lanes], ext[pl.ds(n, 1), lanes]
            below = jnp.where(c == 0, outer, inner)
            above = jnp.where(c == 0, inner, outer)
            near = near + jnp.where(row == 0, below, pltpu.roll(own, 1, 0))
            near = near + jnp.where(row == CY - 1, above, pltpu.roll(own, CY - 1, 0))
            back, forth = pltpu.roll(own, 1, 1), pltpu.roll(own, 383, 1)
            if parity == 0:
                back = jnp.where(column == 0, 0.0, back)
                forth = jnp.where(column == 383, 0.0, forth)
            else:
                prior = dpad[n + 1, :, pl.ds(pl.multiple_of(at, 128), 128)]
                later = dpad[n + 1, :, pl.ds(pl.multiple_of(at + 512, 128), 128)]
                back = jnp.concatenate(
                    [jnp.where(tile == 0, pltpu.roll(prior, 1, 1), back[:, :128]), back[:, 128:]], axis=1
                )
                forth = jnp.concatenate(
                    [forth[:, :256], jnp.where(tile == 127, pltpu.roll(later, 127, 1), forth[:, 256:])], axis=1
                )
            value = right[pl.ds(rows, CY), lanes] - (6.0 * own - (near + back + forth))
            dec_ref[pl.ds(rows, CY), lanes] = own
            res_ref[pl.ds(rows, CY), lanes] = value
            if parity == 0:
                value = jnp.where((column > 0) & (column < 383), value, 0.0)
            return total + squares(value)

        return lax.fori_loop(0, CX, slab, total, unroll=8)

    def seam(k, total):
        at = layer(0, k) * 384

        def slab(n, total):
            rows = pl.multiple_of(n * CY, 8)
            out = pl.ds(rows, CY)
            front = pl.ds(pl.multiple_of(at, 128), 128)
            prior = pltpu.roll(dpad[n + 1, :, front], 1, 1)
            value = res_ref[out, front] + jnp.where(tile == 0, prior, 0.0)
            res_ref[out, front] = value
            total = total + squares(jnp.where(tile == 0, value, 0.0))
            back = pl.ds(pl.multiple_of(at + 256, 128), 128)
            later = pltpu.roll(dpad[n + 1, :, pl.ds(pl.multiple_of(at + 512, 128), 128)], 127, 1)
            value = res_ref[out, back] + jnp.where(tile == 127, later, 0.0)
            res_ref[out, back] = value
            return total + squares(jnp.where(tile == 127, value, 0.0))

        return lax.fori_loop(0, CX, slab, total, unroll=8)

    total = jnp.zeros((8, 128), F32)
    for phase in range(4):
        count = 32 - (phase == 0)
        block = rbuf.at[pl.ds(0, count)]
        with jax.named_scope("s_wait"):
            pltpu.make_async_copy(block, block, recv_sem.at[phase]).wait()
        with jax.named_scope("s_decode"):
            for k in range(2):
                decode(phase, k)
                if phase % 2 == 1:
                    pair_start(phase // 2, k)
        if phase == 1:
            with jax.named_scope("s_early"):
                for k in range(2):
                    pair_copy(0, k).wait()
                    total = residual(0, k, total)
    with jax.named_scope("s_seam"):
        for k in range(2):
            total = seam(k, total)
    with jax.named_scope("s_pair"):
        for k in range(2):
            pair_copy(1, k).wait()
    with jax.named_scope("s_late"):
        for k in range(2):
            total = residual(1, k, total)

    part[...] = jnp.sum(total, axis=0, keepdims=True)
    parts[me] = part[...]

    everyone = pl.ds(0, PEERS - 1)
    with jax.named_scope("s_sent"):
        pltpu.make_async_copy(sbuf.at[everyone], sbuf.at[everyone], send_sem).wait()
    with jax.named_scope("s_tell"):
        everywhere(
            lambda there: pltpu.make_async_remote_copy(
                part, parts.at[me], sum_send, sum_recv, device_id=there, device_id_type=MESH
            ).start()
        )
    with jax.named_scope("s_sum"):
        pltpu.make_async_copy(parts.at[everyone], parts.at[everyone], sum_recv).wait()
    pltpu.make_async_copy(parts.at[everyone], parts.at[everyone], sum_send).wait()
    whole = jnp.sum(jnp.sum(parts[...], axis=0), axis=1, keepdims=True)
    rms_ref[...] = jnp.sqrt(whole / (PEERS * CELLS * NZ) + 1e-06)


def deliver(dec_ref, res_ref, rms_ref, dec_out, res_out, rms_out, sems):
    copies = []
    for src, dst in ((dec_ref, dec_out), (res_ref, res_out)):
        for n in range(4):
            rows = pl.ds(n * (CELLS // 4), CELLS // 4)
            copies.append(pltpu.make_async_copy(src.at[rows], dst.at[rows], sems.at[len(copies)]))
    copies.insert(0, pltpu.make_async_copy(rms_ref, rms_out, sems.at[8]))
    for copy in copies:
        copy.start()
    for copy in copies:
        copy.wait()


def shards(coefficients, exponents, right_side):
    constants = tables()
    any_space = pl.BlockSpec(memory_space=pltpu.HBM)
    vmem = pl.BlockSpec(memory_space=pltpu.VMEM)
    right = right_side.reshape(CELLS, NZ)
    operands = (coefficients, exponents, right, *constants)
    operands = tuple(pltpu.with_memory_space_constraint(jnp.asarray(o), pltpu.HBM) for o in operands)
    held = [pltpu.VMEM(o.shape, o.dtype) for o in operands]
    sem = pltpu.SemaphoreType
    field = jax.ShapeDtypeStruct((CELLS, NZ), F32)
    decoded, residual, rms = pl.pallas_call(
        kernel,
        name="exchange",
        out_shape=(field, field, jax.ShapeDtypeStruct((1, 1), F32)),
        in_specs=[any_space] * len(operands),
        out_specs=(vmem, vmem, vmem),
        scratch_shapes=[
            *held,
            pltpu.VMEM((PEERS, ROWS, CELLS), BF16),
            pltpu.VMEM((PEERS, ROWS, CELLS), BF16),
            pltpu.VMEM((10, 18, 8, 256), F32),
            pltpu.VMEM((CX + 2, CY, NZ + 256), F32),
            pltpu.VMEM((CX, NZ), F32),
            pltpu.VMEM((CX, NZ), F32),
            pltpu.VMEM((CX, NZ), F32),
            pltpu.VMEM((1, 128), F32),
            pltpu.VMEM((PEERS, 1, 128), F32),
            sem.DMA((13,)),
            sem.DMA,
            sem.DMA((4,)),
            sem.DMA((4,)),
            sem.DMA((4,)),
            sem.DMA,
            sem.DMA,
        ],
        compiler_params=pltpu.CompilerParams(collective_id=0, has_side_effects=True, vmem_limit_bytes=VMEM_BYTES),
    )(*operands)
    shape = (CX, CY, NZ)
    decoded, residual, rms = pl.pallas_call(
        deliver,
        name="deliver",
        out_shape=(field, field, jax.ShapeDtypeStruct((1, 1), F32)),
        in_specs=(vmem, vmem, vmem),
        out_specs=(any_space, any_space, any_space),
        scratch_shapes=[sem.DMA((9,))],
        compiler_params=pltpu.CompilerParams(vmem_limit_bytes=1 << 20),
    )(decoded, residual, rms)
    return decoded.reshape(shape), residual.reshape(shape), rms[0, 0]


def solution(mesh):
    placed = (P(("px", "py"), None), P(("px", "py"), None), P("px", "py", None))
    return jax.shard_map(
        shards,
        mesh=mesh,
        in_specs=placed,
        out_specs=(P("px", "py", None), P("px", "py", None), P()),
        check_vma=False,
    )
```

```python
import random

import jax
import jax.numpy as jnp
import numpy as np
from jax import lax
from jax.experimental import pallas as pl
from jax.experimental.pallas import tpu as pltpu
from jax.sharding import PartitionSpec as P

CX = 16
CY = 24
CELLS = CX * CY
NZ = 1536
PEERS = 128
LAYERS = 12
CHUNK = CELLS * PEERS // 4
ROWS = 16
F32 = jnp.float32
BF16 = jnp.bfloat16
MESH = pl.DeviceIdType.MESH
VMEM_BYTES = 40 << 20


def basis():
    a = np.arange(4.0)[:, None]
    i = np.arange(4.0)[None, :]
    weight = np.where(a == 0, np.sqrt(0.25), np.sqrt(0.5))
    return weight * np.cos(np.pi * (2 * i + 1) * a / 8)


def halves(table):
    hi = table.astype(np.float32).astype(BF16)
    lo = (table - hi.astype(np.float64)).astype(np.float32).astype(BF16)
    return hi, lo


def whole_basis():
    b = basis()
    p, q = 408 / 512, 169 / 512
    gain = np.sqrt(b[1, 0] / p * b[1, 1] / q)
    return np.stack([b[0], [p, q, -q, -p], b[2], [q, -p, p, -q]]), gain


def block_table(width):
    b = basis()
    n = np.arange(width)
    return np.where(n[:, None] // 4 == n[None, :] // 4, b[n[:, None] % 4, n[None, :] % 4], 0.0)


def tables():
    b = basis()
    plane = np.kron(block_table(CX), block_table(CY))
    plane_hi, plane_lo = halves(plane.T)
    lane_of = np.zeros((3, 64), np.int64)
    cell_of = np.zeros(256, np.int64)
    part_of = np.full(256, -1)
    for k in range(3):
        for e in range(64):
            lane_of[k, e] = k * 48 + e if e < 48 else 144 + k * 16 + e - 48
        for e in range(24):
            cell_of[k * 48 + e] = e
            cell_of[k * 48 + 24 + e] = 15 * CY + e
        for x in range(16):
            cell_of[144 + k * 16 + x] = x * CY
            cell_of[192 + k * 16 + x] = x * CY + 23
        for first, size in ((k * 48, 48), (144 + k * 16, 16), (192 + k * 16, 16)):
            part_of[first : first + size] = k
    edge = np.where(part_of[None, :] >= 0, plane[:, cell_of], 0.0)
    edge_hi, edge_lo = halves(edge)
    part = np.broadcast_to(part_of[None, :], (8, 256)).astype(np.int32)
    turn = np.zeros((4, 8, 128), np.float32)
    for s in range(4):
        for r in range(4, 8):
            turn[s, r, :] = b[(r + s) % 4, r % 4]
    pick = np.zeros((192, 256))
    for k in range(3):
        for e in range(64):
            pick[k * 64 + e, lane_of[k, e]] = 1
    pick_hi = pick.astype(BF16)
    pick_lo = np.roll(pick, 64, axis=1).astype(BF16)
    left = np.stack(
        [
            np.concatenate([plane_hi[:192, :256], plane_lo[:192, :256], pick_hi]),
            np.concatenate([plane_hi[192:, 128:], plane_lo[192:, 128:], pick_lo]),
        ]
    )
    whole, gain = whole_basis()
    depth = np.zeros((2, 256, 256))
    place = np.zeros((2, 768, 256))
    for odd in range(2):
        for s in range(16):
            base = 64 * odd + s * LAYERS
            for z in range(LAYERS):
                for o in range(z // 4 * 4, z // 4 * 4 + 4):
                    depth[odd, s * 16 + z, base + o] = whole[z % 4, o % 4]
            for k in range(3):
                for r in range(4):
                    place[odd, k * 256 + s * 16 + 12 + r, base + k * 4 + r] = 1
    lift = np.broadcast_to(np.where(np.arange(256) % 2, gain, 1.0)[None, :], (8, 256)).astype(np.float32)
    column = np.arange(CELLS)
    spread = column[:, None] % 24 == (column[None, :] // CY // 4) * 6 + column[None, :] % CY // 4
    spread = np.stack([spread[:256], spread[128:]]).astype(BF16)
    return (
        spread,
        np.concatenate([edge_hi, edge_lo], axis=1),
        part,
        turn,
        left,
        lift,
        depth.astype(BF16),
        place.astype(BF16),
    )


def dot(a, b):
    return lax.dot_general(a, b, (((1,), (0,)), ((), ())), preferred_element_type=F32)


def dot_rows(a, b):
    return lax.dot_general(a, b, (((1,), (1,)), ((), ())), preferred_element_type=F32)


def two(x):
    hi = x.astype(BF16)
    return hi, (x - hi.astype(F32)).astype(BF16)


def position():
    i, j = lax.axis_index("px"), lax.axis_index("py")
    return ((j >> 1) & 1) * 2 + (i & 1), i >> 1, j >> 2, j & 1


def orders():
    every = [(i, j, k, m) for k in range(4) for j in range(4) for i in range(4) for m in range(2)]
    every = every[1:] if every[0] == (0, 0, 0, 0) else every
    random.Random(0).shuffle(every)
    every.sort(key=lambda d: -sum(min(v, 4 - v) for v in d[:3]))
    return [[d for d in every if d[0] % 2 == phase % 2 and d[1] % 2 == phase // 2] for phase in range(4)]


def half_of(distance):
    return (-distance[1] % 4 - distance[1] % 2) // 2


class Peers:
    def __init__(self):
        x, y, z, c = position()
        xs = [(x + d) & 3 for d in range(4)]
        self.x_low = [v & 1 for v in xs]
        self.x_high = [v & 2 for v in xs]
        self.y_part = [((y + d) & 3) * 2 for d in range(4)]
        self.z = z
        self.y = y
        self.core = [c, 1 - c]

    def z_part(self, d):
        return ((self.z + d) & 3) * 4

    def at(self, dx, dy, dz, dc):
        y = self.y_part[dy] if isinstance(dy, int) else ((self.y + dy) & 3) * 2
        return y + self.x_low[dx], self.z_part(dz) + self.x_high[dx] + self.core[dc]


def ident(pair):
    return {"px": pair[0], "py": pair[1]}


def kernel(
    coef_hbm, expo_hbm, right_hbm, spread_hbm, edge_hbm, part_hbm, turn_hbm, left_hbm, lift_hbm, depth_hbm, place_hbm,
    dec_ref, res_ref, sum_ref,
    coef, expo, right, spread, edge, part_of, turn, left, lift, depth, place,
    sbuf, rbuf, ebuf, dpad, ext, pair_out, pair_in, part, parts,
    load_sem, send_sem, recv_sem, pair_send, pair_recv, sum_send, sum_recv,
):
    x, y, z, c = position()
    peers = Peers()
    me = lax.axis_index("px") * 16 + lax.axis_index("py")
    def load(n, src, dst):
        return pltpu.make_async_copy(src, dst, load_sem.at[n])

    chunks = [
        load(n, coef_hbm.at[:, pl.ds(n * CHUNK, CHUNK)], coef.at[:, pl.ds(n * CHUNK, CHUNK)])
        for n in range(4)
    ]
    first = [load(4, expo_hbm, expo), load(5, spread_hbm, spread)]
    second = [load(6, edge_hbm, edge), load(7, part_hbm, part_of), load(8, turn_hbm, turn)]
    third = [load(9, left_hbm, left), load(10, depth_hbm, depth), load(11, place_hbm, place)]
    third += [load(12, lift_hbm, lift), load(13, right_hbm, right)]
    for copy in [*first, *chunks, *second]:
        copy.start()

    entry = pltpu.get_barrier_semaphore()
    def everywhere(act):
        def one(i, _):
            for j in range(8):
                def go(j=j):
                    act(ident(peers.at((2, 1, 3, 0)[j >> 1], i + 2, (i >> 2) + 2, 1 - (j & 1))))

                if j == 7:
                    pl.when(i != 10)(go)
                else:
                    go()
            return 0

        lax.fori_loop(0, 16, one, 0)

    with jax.named_scope("s_signal"):
        everywhere(lambda there: pl.semaphore_signal(entry, inc=1, device_id=there, device_id_type=MESH))

    def clear(g, _):
        sbuf[pl.ds(g * 16, 16), 8:16, :] = jnp.zeros((16, 8, CELLS), BF16)
        ebuf[g + 1, 0] = jnp.zeros((8, 256), F32)
        ebuf[g + 1, 17] = jnp.zeros((8, 256), F32)
        return 0

    lax.fori_loop(0, 8, clear, 0)
    ebuf[0] = jnp.zeros((18, 8, 256), F32)
    ebuf[9] = jnp.zeros((18, 8, 256), F32)

    with jax.named_scope("s_load"):
        for copy in first:
            copy.wait()

    row8 = lax.broadcasted_iota(jnp.int32, (8, 256), 0)
    lane8 = lax.broadcasted_iota(jnp.int32, (8, 256), 1)
    row12 = lax.broadcasted_iota(jnp.int32, (LAYERS, CELLS), 0)
    owners = (lane8 // 24, (lane8 + 128) // 24)
    upper = lax.broadcasted_iota(jnp.int32, (16, 8, 256), 1) < 4

    def scale(h):
        factors = []
        for n in range(2):
            apart = []
            for g in (2 * h, 2 * h + 1):
                at = g * 384 + n * 128
                power = jnp.exp2(expo[:, at : at + 256].astype(F32))
                rows = jnp.where(row8 % 4 == 0, power[0:1], jnp.where(row8 % 4 == 1, power[1:2], power[2:3]))
                apart += [jnp.where(owners[n] == n * 8 + j + row8 // 4, rows, 0.0) for j in range(0, 8, 2)]
            factors.append(dot(jnp.concatenate(apart, axis=0).astype(BF16), spread[n]))
        for j in range(32):
            at = (h * 32 + j) * CELLS
            held = coef[:, at : at + CELLS].astype(F32)
            row = (j // 16 * 8 + j % 8) * 4
            some = factors[j // 8 % 2][row : row + 3]
            factor = jnp.where(row12 < 4, some[0:1], jnp.where(row12 < 8, some[1:2], some[2:3]))
            sbuf[h * 32 + j, 0:LAYERS, :] = (held * factor).astype(BF16)

    def edges(h):
        held = sbuf[h * 32 : h * 32 + 32].reshape(512, CELLS)
        both = dot(held, edge[...])
        both = (both[:, :256] + both[:, 256:]).reshape(32, ROWS, 256)
        kind = part_of[...][None]
        weights = [jnp.concatenate([turn[s], turn[s]], axis=1)[None] for s in range(4)]
        for n in range(2):
            wide = both[n * 16 : n * 16 + 16]
            first, second = wide[:, :8], wide[:, 8:]
            first_turned, second_turned = pltpu.roll(first, 4, 1), pltpu.roll(second, 4, 1)
            four = jnp.where(
                kind == 0,
                jnp.where(upper, first, first_turned),
                jnp.where(
                    kind == 1, jnp.where(upper, first_turned, first), jnp.where(upper, second, second_turned)
                ),
            )
            mixed = four * weights[0]
            for s in range(1, 4):
                mixed = mixed + pltpu.roll(four, 8 - s, 1) * weights[s]
            ebuf[h * 2 + n + 1, 1:17] = mixed

    with jax.named_scope("s_scale"):
        for h in range(4):
            chunks[h].wait()
            scale(h)

    for copy in third:
        copy.start()
    for copy in second:
        copy.wait()

    with jax.named_scope("s_edges"):
        for h in range(4):
            edges(h)

    lane = lax.broadcasted_iota(jnp.int32, (16, 8, 256), 2)
    low = lane % 48 < 24
    across = lane < 144
    half = lax.broadcasted_iota(jnp.int32, (16, 8, 128), 2) < 64
    even = lax.broadcasted_iota(jnp.int32, (16, 8, 128), 0) % 2 == 0

    def layer(parity, k):
        return (y + parity + 2 * k) & 3

    def gather(g):
        value = jnp.where(low, ebuf[g + 2, 1:17], ebuf[g, 1:17])
        along = jnp.where(even, pltpu.roll(ebuf[g + 1, 0:16, :, 128:], 80, 2), ebuf[g + 1, 2:18, :, 128:])
        one = value[:, :, :128]
        two_ = jnp.where(across[:, :, 128:], value[:, :, 128:], along)
        one_hi = one.astype(BF16).astype(F32)
        two_hi = two_.astype(BF16).astype(F32)
        first = pltpu.roll(one - one_hi, 64, 2)
        second = pltpu.roll(two_ - two_hi, 64, 2)
        line = jnp.concatenate([one_hi, jnp.where(half, two_hi, first), jnp.where(half, first, second)], axis=2)
        tall = jnp.concatenate([jnp.zeros((16, 8, CELLS), F32), line], axis=1).astype(BF16)
        sbuf[pl.ds(g * 16, 16)] = sbuf[pl.ds(g * 16, 16)] + tall

    def collect(phase):
        for k in range(2):
            gather(layer(phase // 2, k) * 2 + ((x + phase) & 1))

    def start(phase):
        for distance in orders()[phase]:
            there = peers.at(*distance)
            pltpu.make_async_remote_copy(
                sbuf.at[there[0] * 16 + there[1]], rbuf.at[me], send_sem, recv_sem.at[phase * 2 + half_of(distance)],
                device_id=ident(there), device_id_type=MESH,
            ).start()

    with jax.named_scope("s_gather"):
        collect(0)
        collect(1)
    with jax.named_scope("s_bar"):
        pl.semaphore_wait(entry, PEERS - 1)
    with jax.named_scope("s_start"):
        start(0)
        collect(2)
        start(1)
        collect(3)
        start(2)
        rbuf[me] = sbuf[me]
        start(3)

    for copy in third:
        copy.wait()

    def wipe(n, _):
        dpad[n] = jnp.zeros((CY, NZ + 256), F32)
        return 0

    lax.fori_loop(0, CX + 2, wipe, 0)
    ext[...] = jnp.zeros((CX, NZ), F32)

    here = ident(peers.at(0, 0, 0, 1))

    def pair_copy(parity, k):
        at = pl.multiple_of(layer(parity, k) * 384, 128)
        n = parity * 2 + k
        return pltpu.make_async_remote_copy(
            pair_out.at[:, pl.ds(at, 384)], pair_in.at[:, pl.ds(at, 384)], pair_send.at[n], pair_recv.at[n],
            device_id=here, device_id_type=MESH,
        )

    def pair_start(parity, k):
        at = layer(parity, k) * 384
        lanes = pl.ds(pl.multiple_of(at + 128, 128), 384)
        last = dpad[1 : CX + 1, CY - 8 :, lanes][:, 7, :]
        first = dpad[1 : CX + 1, 0:8, lanes][:, 0, :]
        pair_out[:, pl.ds(pl.multiple_of(at, 128), 384)] = jnp.where(c == 0, last, first)
        pair_copy(parity, k).start()

    def decode(phase, ks):
        odd = (x + phase) & 1
        wides = []
        for k in ks:
            held = rbuf[pl.ds((layer(phase // 2, k) * 2 + odd) * 16, 16)].reshape(256, CELLS)
            wides.append((dot_rows(left[0], held[:, :256]), dot_rows(left[1], held[:, 128:])))
        for k, (near, far) in zip(ks, wides):
            across = jnp.concatenate([near[:192] + near[192:384], far[:192] + far[192:384]], axis=0)
            hi, lo = two(across * lift[0:1, :])
            field = dot(hi, depth[odd]) + dot(lo, depth[odd])
            side_hi = jnp.concatenate([near[384:448], near[448:512], near[512:576]], axis=1).astype(BF16)
            side_lo = jnp.concatenate([far[384:448], far[448:512], far[512:576]], axis=1).astype(BF16)
            side = dot(jnp.concatenate([side_hi, side_lo], axis=0), place[odd])
            side = side[:64] + side[64:]
            at = layer(phase // 2, k) * 384 + odd * 128
            lanes = pl.ds(pl.multiple_of(at + 128, 128), 256)
            dpad[1 : CX + 1, :, lanes] += field.reshape(CX, CY, 256)
            dpad[0, :, lanes] += side[24:48]
            dpad[CX + 1, :, lanes] += side[0:24]
            ext[:, pl.ds(pl.multiple_of(at, 128), 256)] += side[48:64]
            if phase % 2 == 1:
                pair_start(phase // 2, k)

    column = lax.broadcasted_iota(jnp.int32, (CY, 384), 1)
    row = lax.broadcasted_iota(jnp.int32, (CY, 384), 0)
    tile = lax.broadcasted_iota(jnp.int32, (CY, 128), 1)

    def squares(value):
        value = value * value
        value = value[0:8] + value[8:16] + value[16:24]
        return sum(value[:, k * 128 : (k + 1) * 128] for k in range(value.shape[1] // 128))

    def residual(parity, k, total):
        depth_at = layer(parity, k)
        at = depth_at * 384
        lanes = pl.ds(pl.multiple_of(at, 128), 384)
        inside = pl.ds(pl.multiple_of(at + 128, 128), 384)
        low_at = jnp.maximum(at - 128, 0)
        high_at = jnp.minimum(at + 384, NZ - 128)
        counted = ((column > 0) | (depth_at == 0)) & ((column < 383) | (depth_at == 3))

        def slab(n, total):
            rows = pl.ds(pl.multiple_of(n * CY, 8), CY)
            own = dpad[n + 1, :, inside]
            near = dpad[n, :, inside] + dpad[n + 2, :, inside]
            inner, outer = pair_in[pl.ds(n, 1), lanes], ext[pl.ds(n, 1), lanes]
            below = jnp.where(c == 0, outer, inner)
            above = jnp.where(c == 0, inner, outer)
            near = near + jnp.where(row == 0, below, pltpu.roll(own, 1, 0))
            near = near + jnp.where(row == CY - 1, above, pltpu.roll(own, CY - 1, 0))
            back, forth = pltpu.roll(own, 1, 1), pltpu.roll(own, 383, 1)
            if parity == 0:
                back = jnp.where(column == 0, 0.0, back)
                forth = jnp.where(column == 383, 0.0, forth)
            else:
                prior = dpad[n + 1, :, pl.ds(pl.multiple_of(at, 128), 128)]
                later = dpad[n + 1, :, pl.ds(pl.multiple_of(at + 512, 128), 128)]
                first, last = back[:, :128], forth[:, 256:]
                back = jnp.concatenate([jnp.where(tile == 0, pltpu.roll(prior, 1, 1), first), back[:, 128:]], axis=1)
                forth = jnp.concatenate(
                    [forth[:, :256], jnp.where(tile == 127, pltpu.roll(later, 127, 1), last)], axis=1
                )
            value = right[rows, lanes] - (6.0 * own - (near + back + forth))
            dec_ref[rows, lanes] = own
            res_ref[rows, lanes] = value
            if parity == 0:
                return total + squares(jnp.where(counted, value, 0.0))
            total = total + squares(value)
            for there, edge_lane, carried, exists in (
                (low_at, 127, last, depth_at > 0),
                (high_at, 0, first, depth_at < 3),
            ):
                spot = pl.ds(pl.multiple_of(there, 128), 128)
                mine = (tile == edge_lane) & exists
                value = res_ref[rows, spot] + jnp.where(mine, carried, 0.0)
                res_ref[rows, spot] = value
                total = total + squares(jnp.where(mine, value, 0.0))
            return total

        return lax.fori_loop(0, CX, slab, total, unroll=8)

    total = jnp.zeros((8, 128), F32)
    for phase in range(4):
        def arrive(k):
            block = rbuf.at[pl.ds(0, 16 - (phase == 0 and k == 0))]
            with jax.named_scope("s_wait"):
                pltpu.make_async_copy(block, block, recv_sem.at[phase * 2 + k]).wait()

        if phase == 3:
            arrive(0)
            arrive(1)
            with jax.named_scope("s_decode"):
                decode(phase, (0, 1))
        else:
            for k in range(2):
                arrive(k)
                with jax.named_scope("s_decode"):
                    decode(phase, (k,))
        if phase == 1:
            with jax.named_scope("s_early"):
                for k in range(2):
                    pair_copy(0, k).wait()
                    total = residual(0, k, total)
    for k in range(2):
        with jax.named_scope("s_pair"):
            pair_copy(1, k).wait()
        with jax.named_scope("s_late"):
            total = residual(1, k, total)

    part[...] = jnp.sum(total, axis=0, keepdims=True)
    parts[me] = part[...]

    everyone = pl.ds(0, PEERS - 1)
    with jax.named_scope("s_sent"):
        pltpu.make_async_copy(sbuf.at[everyone], sbuf.at[everyone], send_sem).wait()
    with jax.named_scope("s_tell"):
        everywhere(
            lambda there: pltpu.make_async_remote_copy(
                part, parts.at[me], sum_send, sum_recv, device_id=there, device_id_type=MESH
            ).start()
        )
    with jax.named_scope("s_sum"):
        pltpu.make_async_copy(parts.at[everyone], parts.at[everyone], sum_recv).wait()
    pltpu.make_async_copy(parts.at[everyone], parts.at[everyone], sum_send).wait()
    sum_ref[...] = jnp.broadcast_to(jnp.sum(parts[...], axis=0), (8, 128))


def deliver(dec_ref, res_ref, sum_ref, dec_out, res_out, rms_out, rms, sems):
    copies = [
        pltpu.make_async_copy(src, dst, sems.at[n])
        for n, (src, dst) in enumerate(((dec_ref, dec_out), (res_ref, res_out), (rms, rms_out)))
    ]
    copies[0].start()
    copies[1].start()
    whole = jnp.sum(sum_ref[0:1, :], axis=1, keepdims=True)
    rms[...] = jnp.sqrt(whole / (PEERS * CELLS * NZ) + 1e-06)
    copies[2].start()
    for copy in copies:
        copy.wait()


def shards(coefficients, exponents, right_side):
    constants = tables()
    any_space = pl.BlockSpec(memory_space=pltpu.HBM)
    vmem = pl.BlockSpec(memory_space=pltpu.VMEM)
    right = right_side.reshape(CELLS, NZ)
    operands = (coefficients, exponents, right, *constants)
    operands = tuple(pltpu.with_memory_space_constraint(jnp.asarray(o), pltpu.HBM) for o in operands)
    held = [pltpu.VMEM(o.shape, o.dtype) for o in operands]
    sem = pltpu.SemaphoreType
    field = jax.ShapeDtypeStruct((CELLS, NZ), F32)
    decoded, residual, total = pl.pallas_call(
        kernel,
        name="exchange",
        out_shape=(field, field, jax.ShapeDtypeStruct((8, 128), F32)),
        in_specs=[any_space] * len(operands),
        out_specs=(vmem, vmem, vmem),
        scratch_shapes=[
            *held,
            pltpu.VMEM((PEERS, ROWS, CELLS), BF16),
            pltpu.VMEM((PEERS, ROWS, CELLS), BF16),
            pltpu.VMEM((10, 18, 8, 256), F32),
            pltpu.VMEM((CX + 2, CY, NZ + 256), F32),
            pltpu.VMEM((CX, NZ), F32),
            pltpu.VMEM((CX, NZ), F32),
            pltpu.VMEM((CX, NZ), F32),
            pltpu.VMEM((1, 128), F32),
            pltpu.VMEM((PEERS, 1, 128), F32),
            sem.DMA((14,)),
            sem.DMA,
            sem.DMA((8,)),
            sem.DMA((4,)),
            sem.DMA((4,)),
            sem.DMA,
            sem.DMA,
        ],
        compiler_params=pltpu.CompilerParams(collective_id=0, has_side_effects=True, vmem_limit_bytes=VMEM_BYTES),
    )(*operands)
    shape = (CX, CY, NZ)
    decoded, residual, rms = pl.pallas_call(
        deliver,
        name="deliver",
        out_shape=(field, field, jax.ShapeDtypeStruct((1, 1), F32)),
        in_specs=(vmem, vmem, vmem),
        out_specs=(any_space, any_space, any_space),
        scratch_shapes=[pltpu.VMEM((1, 1), F32), sem.DMA((3,))],
        compiler_params=pltpu.CompilerParams(vmem_limit_bytes=1 << 20),
    )(decoded, residual, total)
    return decoded.reshape(shape), residual.reshape(shape), rms[0, 0]


def solution(mesh):
    placed = (P(("px", "py"), None), P(("px", "py"), None), P("px", "py", None))
    return jax.shard_map(
        shards,
        mesh=mesh,
        in_specs=placed,
        out_specs=(P("px", "py", None), P("px", "py", None), P()),
        check_vma=False,
    )
```

```python
import random

import jax
import jax.numpy as jnp
import numpy as np
from jax import lax
from jax.experimental import pallas as pl
from jax.experimental.pallas import tpu as pltpu
from jax.sharding import PartitionSpec as P

CX = 16
CY = 24
CELLS = CX * CY
NZ = 1536
PEERS = 128
LAYERS = 12
CHUNK = CELLS * PEERS // 4
ROWS = 16
F32 = jnp.float32
BF16 = jnp.bfloat16
MESH = pl.DeviceIdType.MESH
VMEM_BYTES = 40 << 20


def basis():
    a = np.arange(4.0)[:, None]
    i = np.arange(4.0)[None, :]
    weight = np.where(a == 0, np.sqrt(0.25), np.sqrt(0.5))
    return weight * np.cos(np.pi * (2 * i + 1) * a / 8)


def halves(table):
    hi = table.astype(np.float32).astype(BF16)
    lo = (table - hi.astype(np.float64)).astype(np.float32).astype(BF16)
    return hi, lo


def whole_basis():
    b = basis()
    p, q = 408 / 512, 169 / 512
    gain = np.sqrt(b[1, 0] / p * b[1, 1] / q)
    return np.stack([b[0], [p, q, -q, -p], b[2], [q, -p, p, -q]]), gain


def block_table(width):
    b = basis()
    n = np.arange(width)
    return np.where(n[:, None] // 4 == n[None, :] // 4, b[n[:, None] % 4, n[None, :] % 4], 0.0)


def tables():
    b = basis()
    plane = np.kron(block_table(CX), block_table(CY))
    plane_hi, plane_lo = halves(plane.T)
    lane_of = np.zeros((3, 64), np.int64)
    cell_of = np.zeros(256, np.int64)
    part_of = np.full(256, -1)
    for k in range(3):
        for e in range(64):
            lane_of[k, e] = k * 48 + e if e < 48 else 144 + k * 16 + e - 48
        for e in range(24):
            cell_of[k * 48 + e] = e
            cell_of[k * 48 + 24 + e] = 15 * CY + e
        for x in range(16):
            cell_of[144 + k * 16 + x] = x * CY
            cell_of[192 + k * 16 + x] = x * CY + 23
        for first, size in ((k * 48, 48), (144 + k * 16, 16), (192 + k * 16, 16)):
            part_of[first : first + size] = k
    edge = np.where(part_of[None, :] >= 0, plane[:, cell_of], 0.0)
    edge_hi, edge_lo = halves(edge)
    part = np.broadcast_to(part_of[None, :], (8, 256)).astype(np.int32)
    turn = np.zeros((4, 8, 128), np.float32)
    for s in range(4):
        for r in range(4, 8):
            turn[s, r, :] = b[(r + s) % 4, r % 4]
    pick = np.zeros((192, 256))
    for k in range(3):
        for e in range(64):
            pick[k * 64 + e, lane_of[k, e]] = 1
    pick_hi = pick.astype(BF16)
    pick_lo = np.roll(pick, 64, axis=1).astype(BF16)
    left = np.stack(
        [
            np.concatenate([plane_hi[:192, :256], plane_lo[:192, :256], pick_hi]),
            np.concatenate([plane_hi[192:, 128:], plane_lo[192:, 128:], pick_lo]),
        ]
    )
    whole, gain = whole_basis()
    depth = np.zeros((2, 256, 256))
    place = np.zeros((2, 768, 256))
    for odd in range(2):
        for s in range(16):
            base = 64 * odd + s * LAYERS
            for z in range(LAYERS):
                for o in range(z // 4 * 4, z // 4 * 4 + 4):
                    depth[odd, s * 16 + z, base + o] = whole[z % 4, o % 4]
            for k in range(3):
                for r in range(4):
                    place[odd, k * 256 + s * 16 + 12 + r, base + k * 4 + r] = 1
    lift = np.broadcast_to(np.where(np.arange(256) % 2, gain, 1.0)[None, :], (8, 256)).astype(np.float32)
    column = np.arange(CELLS)
    spread = column[:, None] % 24 == (column[None, :] // CY // 4) * 6 + column[None, :] % CY // 4
    spread = np.stack([spread[:256], spread[128:]]).astype(BF16)
    return (
        spread,
        np.concatenate([edge_hi, edge_lo], axis=1),
        part,
        turn,
        left,
        lift,
        depth.astype(BF16),
        place.astype(BF16),
    )


def dot(a, b):
    return lax.dot_general(a, b, (((1,), (0,)), ((), ())), preferred_element_type=F32)


def dot_rows(a, b):
    return lax.dot_general(a, b, (((1,), (1,)), ((), ())), preferred_element_type=F32)


def two(x):
    hi = x.astype(BF16)
    return hi, (x - hi.astype(F32)).astype(BF16)


def position():
    i, j = lax.axis_index("px"), lax.axis_index("py")
    return ((j >> 1) & 1) * 2 + (i & 1), i >> 1, j >> 2, j & 1


def orders():
    every = [(i, j, k, m) for k in range(4) for j in range(4) for i in range(4) for m in range(2)]
    every = every[1:] if every[0] == (0, 0, 0, 0) else every
    random.Random(0).shuffle(every)
    every.sort(key=lambda d: -sum(min(v, 4 - v) for v in d[:3]))
    return [[d for d in every if d[0] % 2 == phase % 2 and d[1] % 2 == phase // 2] for phase in range(4)]


def half_of(distance):
    return (-distance[1] % 4 - distance[1] % 2) // 2


class Peers:
    def __init__(self):
        x, y, z, c = position()
        xs = [(x + d) & 3 for d in range(4)]
        self.x_low = [v & 1 for v in xs]
        self.x_high = [v & 2 for v in xs]
        self.y_part = [((y + d) & 3) * 2 for d in range(4)]
        self.z = z
        self.y = y
        self.core = [c, 1 - c]

    def z_part(self, d):
        return ((self.z + d) & 3) * 4

    def at(self, dx, dy, dz, dc):
        y = self.y_part[dy] if isinstance(dy, int) else ((self.y + dy) & 3) * 2
        return y + self.x_low[dx], self.z_part(dz) + self.x_high[dx] + self.core[dc]


def ident(pair):
    return {"px": pair[0], "py": pair[1]}


def kernel(
    coef_hbm, expo_hbm, right_hbm, spread_hbm, edge_hbm, part_hbm, turn_hbm, left_hbm, lift_hbm, depth_hbm, place_hbm,
    dec_ref, res_ref, sum_ref,
    coef, expo, right, spread, edge, part_of, turn, left, lift, depth, place,
    sbuf, rbuf, ebuf, dpad, ext, pair_out, pair_in, part, parts,
    load_sem, send_sem, recv_sem, pair_send, pair_recv, sum_send, sum_recv,
):
    x, y, z, c = position()
    peers = Peers()
    me = lax.axis_index("px") * 16 + lax.axis_index("py")
    def load(n, src, dst):
        return pltpu.make_async_copy(src, dst, load_sem.at[n])

    chunks = [
        load(n, coef_hbm.at[:, pl.ds(n * CHUNK, CHUNK)], coef.at[:, pl.ds(n * CHUNK, CHUNK)])
        for n in range(4)
    ]
    first = [load(4, expo_hbm, expo), load(5, spread_hbm, spread)]
    second = [load(6, edge_hbm, edge), load(7, part_hbm, part_of), load(8, turn_hbm, turn)]
    third = [load(9, left_hbm, left), load(10, depth_hbm, depth), load(11, place_hbm, place)]
    third += [load(12, lift_hbm, lift), load(13, right_hbm, right)]
    for copy in [*first, *chunks, *second]:
        copy.start()

    entry = pltpu.get_barrier_semaphore()
    def everywhere(act):
        for distance in sorted(sum(orders(), []), key=lambda d: -sum(min(v, 4 - v) for v in d[:3])):
            act(ident(peers.at(*distance)))

    with jax.named_scope("s_signal"):
        everywhere(lambda there: pl.semaphore_signal(entry, inc=1, device_id=there, device_id_type=MESH))

    def clear(g, _):
        sbuf[pl.ds(g * 16, 16), 8:16, :] = jnp.zeros((16, 8, CELLS), BF16)
        ebuf[g + 1, 0] = jnp.zeros((8, 256), F32)
        ebuf[g + 1, 17] = jnp.zeros((8, 256), F32)
        return 0

    lax.fori_loop(0, 8, clear, 0)
    ebuf[0] = jnp.zeros((18, 8, 256), F32)
    ebuf[9] = jnp.zeros((18, 8, 256), F32)

    with jax.named_scope("s_load"):
        for copy in first:
            copy.wait()

    row8 = lax.broadcasted_iota(jnp.int32, (8, 256), 0)
    lane8 = lax.broadcasted_iota(jnp.int32, (8, 256), 1)
    row12 = lax.broadcasted_iota(jnp.int32, (LAYERS, CELLS), 0)
    owners = (lane8 // 24, (lane8 + 128) // 24)
    upper = lax.broadcasted_iota(jnp.int32, (16, 8, 256), 1) < 4

    def scale(h):
        factors = []
        for n in range(2):
            apart = []
            for g in (2 * h, 2 * h + 1):
                at = g * 384 + n * 128
                power = jnp.exp2(expo[:, at : at + 256].astype(F32))
                rows = jnp.where(row8 % 4 == 0, power[0:1], jnp.where(row8 % 4 == 1, power[1:2], power[2:3]))
                apart += [jnp.where(owners[n] == n * 8 + j + row8 // 4, rows, 0.0) for j in range(0, 8, 2)]
            factors.append(dot(jnp.concatenate(apart, axis=0).astype(BF16), spread[n]))
        for j in range(32):
            at = (h * 32 + j) * CELLS
            held = coef[:, at : at + CELLS].astype(F32)
            row = (j // 16 * 8 + j % 8) * 4
            some = factors[j // 8 % 2][row : row + 3]
            factor = jnp.where(row12 < 4, some[0:1], jnp.where(row12 < 8, some[1:2], some[2:3]))
            sbuf[h * 32 + j, 0:LAYERS, :] = (held * factor).astype(BF16)

    def edges(h):
        held = sbuf[h * 32 : h * 32 + 32].reshape(512, CELLS)
        both = dot(held, edge[...])
        both = (both[:, :256] + both[:, 256:]).reshape(32, ROWS, 256)
        kind = part_of[...][None]
        weights = [jnp.concatenate([turn[s], turn[s]], axis=1)[None] for s in range(4)]
        for n in range(2):
            wide = both[n * 16 : n * 16 + 16]
            first, second = wide[:, :8], wide[:, 8:]
            first_turned, second_turned = pltpu.roll(first, 4, 1), pltpu.roll(second, 4, 1)
            four = jnp.where(
                kind == 0,
                jnp.where(upper, first, first_turned),
                jnp.where(
                    kind == 1, jnp.where(upper, first_turned, first), jnp.where(upper, second, second_turned)
                ),
            )
            mixed = four * weights[0]
            for s in range(1, 4):
                mixed = mixed + pltpu.roll(four, 8 - s, 1) * weights[s]
            ebuf[h * 2 + n + 1, 1:17] = mixed

    with jax.named_scope("s_scale"):
        for h in range(4):
            chunks[h].wait()
            scale(h)

    for copy in third:
        copy.start()
    for copy in second:
        copy.wait()

    with jax.named_scope("s_edges"):
        for h in range(4):
            edges(h)

    lane = lax.broadcasted_iota(jnp.int32, (16, 8, 256), 2)
    low = lane % 48 < 24
    across = lane < 144
    half = lax.broadcasted_iota(jnp.int32, (16, 8, 128), 2) < 64
    even = lax.broadcasted_iota(jnp.int32, (16, 8, 128), 0) % 2 == 0

    def layer(parity, k):
        return (y + parity + 2 * k) & 3

    def gather(g):
        value = jnp.where(low, ebuf[g + 2, 1:17], ebuf[g, 1:17])
        along = jnp.where(even, pltpu.roll(ebuf[g + 1, 0:16, :, 128:], 80, 2), ebuf[g + 1, 2:18, :, 128:])
        one = value[:, :, :128]
        two_ = jnp.where(across[:, :, 128:], value[:, :, 128:], along)
        one_hi = one.astype(BF16).astype(F32)
        two_hi = two_.astype(BF16).astype(F32)
        first = pltpu.roll(one - one_hi, 64, 2)
        second = pltpu.roll(two_ - two_hi, 64, 2)
        line = jnp.concatenate([one_hi, jnp.where(half, two_hi, first), jnp.where(half, first, second)], axis=2)
        tall = jnp.concatenate([jnp.zeros((16, 8, CELLS), F32), line], axis=1).astype(BF16)
        sbuf[pl.ds(g * 16, 16)] = sbuf[pl.ds(g * 16, 16)] + tall

    def collect(phase):
        for k in range(2):
            gather(layer(phase // 2, k) * 2 + ((x + phase) & 1))

    def start(phase):
        for distance in orders()[phase]:
            there = peers.at(*distance)
            pltpu.make_async_remote_copy(
                sbuf.at[there[0] * 16 + there[1]], rbuf.at[me], send_sem, recv_sem.at[phase * 2 + half_of(distance)],
                device_id=ident(there), device_id_type=MESH,
            ).start()

    with jax.named_scope("s_gather"):
        collect(0)
        collect(1)
    with jax.named_scope("s_bar"):
        pl.semaphore_wait(entry, PEERS - 1)
    with jax.named_scope("s_start"):
        start(0)
        collect(2)
        start(1)
        collect(3)
        start(2)
        rbuf[me] = sbuf[me]
        start(3)

    for copy in third:
        copy.wait()

    def wipe(n, _):
        dpad[n] = jnp.zeros((CY, NZ + 256), F32)
        return 0

    lax.fori_loop(0, CX + 2, wipe, 0)
    ext[...] = jnp.zeros((CX, NZ), F32)

    here = ident(peers.at(0, 0, 0, 1))

    def pair_copy(parity, k):
        at = pl.multiple_of(layer(parity, k) * 384, 128)
        n = parity * 2 + k
        return pltpu.make_async_remote_copy(
            pair_out.at[:, pl.ds(at, 384)], pair_in.at[:, pl.ds(at, 384)], pair_send.at[n], pair_recv.at[n],
            device_id=here, device_id_type=MESH,
        )

    def pair_start(parity, k):
        at = layer(parity, k) * 384
        lanes = pl.ds(pl.multiple_of(at + 128, 128), 384)
        last = dpad[1 : CX + 1, CY - 8 :, lanes][:, 7, :]
        first = dpad[1 : CX + 1, 0:8, lanes][:, 0, :]
        pair_out[:, pl.ds(pl.multiple_of(at, 128), 384)] = jnp.where(c == 0, last, first)
        pair_copy(parity, k).start()

    def decode(phase, ks):
        odd = (x + phase) & 1
        wides = []
        for k in ks:
            held = rbuf[pl.ds((layer(phase // 2, k) * 2 + odd) * 16, 16)].reshape(256, CELLS)
            wides.append((dot_rows(left[0], held[:, :256]), dot_rows(left[1], held[:, 128:])))
        for k, (near, far) in zip(ks, wides):
            across = jnp.concatenate([near[:192] + near[192:384], far[:192] + far[192:384]], axis=0)
            hi, lo = two(across * lift[0:1, :])
            field = dot(hi, depth[odd]) + dot(lo, depth[odd])
            side_hi = jnp.concatenate([near[384:448], near[448:512], near[512:576]], axis=1).astype(BF16)
            side_lo = jnp.concatenate([far[384:448], far[448:512], far[512:576]], axis=1).astype(BF16)
            side = dot(jnp.concatenate([side_hi, side_lo], axis=0), place[odd])
            side = side[:64] + side[64:]
            at = layer(phase // 2, k) * 384 + odd * 128
            lanes = pl.ds(pl.multiple_of(at + 128, 128), 256)
            dpad[1 : CX + 1, :, lanes] += field.reshape(CX, CY, 256)
            dpad[0, :, lanes] += side[24:48]
            dpad[CX + 1, :, lanes] += side[0:24]
            ext[:, pl.ds(pl.multiple_of(at, 128), 256)] += side[48:64]
            if phase % 2 == 1:
                pair_start(phase // 2, k)

    column = lax.broadcasted_iota(jnp.int32, (CY, 384), 1)
    row = lax.broadcasted_iota(jnp.int32, (CY, 384), 0)
    tile = lax.broadcasted_iota(jnp.int32, (CY, 128), 1)

    def squares(value):
        value = value * value
        value = value[0:8] + value[8:16] + value[16:24]
        return sum(value[:, k * 128 : (k + 1) * 128] for k in range(value.shape[1] // 128))

    def residual(parity, k, total):
        depth_at = layer(parity, k)
        at = depth_at * 384
        lanes = pl.ds(pl.multiple_of(at, 128), 384)
        inside = pl.ds(pl.multiple_of(at + 128, 128), 384)
        low_at = jnp.maximum(at - 128, 0)
        high_at = jnp.minimum(at + 384, NZ - 128)
        counted = ((column > 0) | (depth_at == 0)) & ((column < 383) | (depth_at == 3))

        def slab(n, total):
            rows = pl.ds(pl.multiple_of(n * CY, 8), CY)
            own = dpad[n + 1, :, inside]
            near = dpad[n, :, inside] + dpad[n + 2, :, inside]
            inner, outer = pair_in[pl.ds(n, 1), lanes], ext[pl.ds(n, 1), lanes]
            below = jnp.where(c == 0, outer, inner)
            above = jnp.where(c == 0, inner, outer)
            near = near + jnp.where(row == 0, below, pltpu.roll(own, 1, 0))
            near = near + jnp.where(row == CY - 1, above, pltpu.roll(own, CY - 1, 0))
            back, forth = pltpu.roll(own, 1, 1), pltpu.roll(own, 383, 1)
            if parity == 0:
                back = jnp.where(column == 0, 0.0, back)
                forth = jnp.where(column == 383, 0.0, forth)
            else:
                prior = dpad[n + 1, :, pl.ds(pl.multiple_of(at, 128), 128)]
                later = dpad[n + 1, :, pl.ds(pl.multiple_of(at + 512, 128), 128)]
                first, last = back[:, :128], forth[:, 256:]
                back = jnp.concatenate([jnp.where(tile == 0, pltpu.roll(prior, 1, 1), first), back[:, 128:]], axis=1)
                forth = jnp.concatenate(
                    [forth[:, :256], jnp.where(tile == 127, pltpu.roll(later, 127, 1), last)], axis=1
                )
            value = right[rows, lanes] - (6.0 * own - (near + back + forth))
            dec_ref[rows, lanes] = own
            res_ref[rows, lanes] = value
            if parity == 0:
                return total + squares(jnp.where(counted, value, 0.0))
            total = total + squares(value)
            for there, edge_lane, carried, exists in (
                (low_at, 127, last, depth_at > 0),
                (high_at, 0, first, depth_at < 3),
            ):
                spot = pl.ds(pl.multiple_of(there, 128), 128)
                mine = (tile == edge_lane) & exists
                value = res_ref[rows, spot] + jnp.where(mine, carried, 0.0)
                res_ref[rows, spot] = value
                total = total + squares(jnp.where(mine, value, 0.0))
            return total

        return lax.fori_loop(0, CX, slab, total, unroll=8)

    total = jnp.zeros((8, 128), F32)
    for phase in range(4):
        def arrive(k):
            block = rbuf.at[pl.ds(0, 16 - (phase == 0 and k == 0))]
            with jax.named_scope("s_wait"):
                pltpu.make_async_copy(block, block, recv_sem.at[phase * 2 + k]).wait()

        if phase == 3:
            arrive(0)
            arrive(1)
            with jax.named_scope("s_decode"):
                decode(phase, (0, 1))
        else:
            for k in range(2):
                arrive(k)
                with jax.named_scope("s_decode"):
                    decode(phase, (k,))
        if phase == 1:
            with jax.named_scope("s_early"):
                for k in range(2):
                    pair_copy(0, k).wait()
                    total = residual(0, k, total)
    for k in range(2):
        with jax.named_scope("s_pair"):
            pair_copy(1, k).wait()
        with jax.named_scope("s_late"):
            total = residual(1, k, total)

    part[...] = jnp.sum(total, axis=0, keepdims=True)
    parts[me] = part[...]

    everyone = pl.ds(0, PEERS - 1)
    with jax.named_scope("s_sent"):
        pltpu.make_async_copy(sbuf.at[everyone], sbuf.at[everyone], send_sem).wait()
    with jax.named_scope("s_tell"):
        everywhere(
            lambda there: pltpu.make_async_remote_copy(
                part, parts.at[me], sum_send, sum_recv, device_id=there, device_id_type=MESH
            ).start()
        )
    with jax.named_scope("s_sum"):
        pltpu.make_async_copy(parts.at[everyone], parts.at[everyone], sum_recv).wait()
    pltpu.make_async_copy(parts.at[everyone], parts.at[everyone], sum_send).wait()
    sum_ref[...] = jnp.broadcast_to(jnp.sum(parts[...], axis=0), (8, 128))


def deliver(dec_ref, res_ref, sum_ref, dec_out, res_out, rms_out, rms, sems):
    copies = [
        pltpu.make_async_copy(src, dst, sems.at[n])
        for n, (src, dst) in enumerate(((dec_ref, dec_out), (res_ref, res_out), (rms, rms_out)))
    ]
    copies[0].start()
    copies[1].start()
    whole = jnp.sum(sum_ref[0:1, :], axis=1, keepdims=True)
    rms[...] = jnp.sqrt(whole / (PEERS * CELLS * NZ) + 1e-06)
    copies[2].start()
    for copy in copies:
        copy.wait()


def shards(coefficients, exponents, right_side):
    constants = tables()
    any_space = pl.BlockSpec(memory_space=pltpu.HBM)
    vmem = pl.BlockSpec(memory_space=pltpu.VMEM)
    right = right_side.reshape(CELLS, NZ)
    operands = (coefficients, exponents, right, *constants)
    operands = tuple(pltpu.with_memory_space_constraint(jnp.asarray(o), pltpu.HBM) for o in operands)
    held = [pltpu.VMEM(o.shape, o.dtype) for o in operands]
    sem = pltpu.SemaphoreType
    field = jax.ShapeDtypeStruct((CELLS, NZ), F32)
    decoded, residual, total = pl.pallas_call(
        kernel,
        name="exchange",
        out_shape=(field, field, jax.ShapeDtypeStruct((8, 128), F32)),
        in_specs=[any_space] * len(operands),
        out_specs=(vmem, vmem, vmem),
        scratch_shapes=[
            *held,
            pltpu.VMEM((PEERS, ROWS, CELLS), BF16),
            pltpu.VMEM((PEERS, ROWS, CELLS), BF16),
            pltpu.VMEM((10, 18, 8, 256), F32),
            pltpu.VMEM((CX + 2, CY, NZ + 256), F32),
            pltpu.VMEM((CX, NZ), F32),
            pltpu.VMEM((CX, NZ), F32),
            pltpu.VMEM((CX, NZ), F32),
            pltpu.VMEM((1, 128), F32),
            pltpu.VMEM((PEERS, 1, 128), F32),
            sem.DMA((14,)),
            sem.DMA,
            sem.DMA((8,)),
            sem.DMA((4,)),
            sem.DMA((4,)),
            sem.DMA,
            sem.DMA,
        ],
        compiler_params=pltpu.CompilerParams(collective_id=0, has_side_effects=True, vmem_limit_bytes=VMEM_BYTES),
    )(*operands)
    shape = (CX, CY, NZ)
    decoded, residual, rms = pl.pallas_call(
        deliver,
        name="deliver",
        out_shape=(field, field, jax.ShapeDtypeStruct((1, 1), F32)),
        in_specs=(vmem, vmem, vmem),
        out_specs=(any_space, any_space, any_space),
        scratch_shapes=[pltpu.VMEM((1, 1), F32), sem.DMA((3,))],
        compiler_params=pltpu.CompilerParams(vmem_limit_bytes=1 << 20),
    )(decoded, residual, total)
    return decoded.reshape(shape), residual.reshape(shape), rms[0, 0]


def solution(mesh):
    placed = (P(("px", "py"), None), P(("px", "py"), None), P("px", "py", None))
    return jax.shard_map(
        shards,
        mesh=mesh,
        in_specs=placed,
        out_specs=(P("px", "py", None), P("px", "py", None), P()),
        check_vma=False,
    )
```

```python
import random

import jax
import jax.numpy as jnp
import numpy as np
from jax import lax
from jax.experimental import pallas as pl
from jax.experimental.pallas import tpu as pltpu
from jax.sharding import PartitionSpec as P

CX = 16
CY = 24
CELLS = CX * CY
NZ = 1536
PEERS = 128
LAYERS = 12
CHUNK = CELLS * PEERS // 4
ROWS = 16
F32 = jnp.float32
BF16 = jnp.bfloat16
MESH = pl.DeviceIdType.MESH
VMEM_BYTES = 40 << 20


def basis():
    a = np.arange(4.0)[:, None]
    i = np.arange(4.0)[None, :]
    weight = np.where(a == 0, np.sqrt(0.25), np.sqrt(0.5))
    return weight * np.cos(np.pi * (2 * i + 1) * a / 8)


def halves(table):
    hi = table.astype(np.float32).astype(BF16)
    lo = (table - hi.astype(np.float64)).astype(np.float32).astype(BF16)
    return hi, lo


def whole_basis():
    b = basis()
    p, q = 408 / 512, 169 / 512
    gain = np.sqrt(b[1, 0] / p * b[1, 1] / q)
    return np.stack([b[0], [p, q, -q, -p], b[2], [q, -p, p, -q]]), gain


def block_table(width):
    b = basis()
    n = np.arange(width)
    return np.where(n[:, None] // 4 == n[None, :] // 4, b[n[:, None] % 4, n[None, :] % 4], 0.0)


def tables():
    b = basis()
    plane = np.kron(block_table(CX), block_table(CY))
    plane_hi, plane_lo = halves(plane.T)
    lane_of = np.zeros((3, 64), np.int64)
    cell_of = np.zeros(256, np.int64)
    part_of = np.full(256, -1)
    for k in range(3):
        for e in range(64):
            lane_of[k, e] = k * 48 + e if e < 48 else 144 + k * 16 + e - 48
        for e in range(24):
            cell_of[k * 48 + e] = e
            cell_of[k * 48 + 24 + e] = 15 * CY + e
        for x in range(16):
            cell_of[144 + k * 16 + x] = x * CY
            cell_of[192 + k * 16 + x] = x * CY + 23
        for first, size in ((k * 48, 48), (144 + k * 16, 16), (192 + k * 16, 16)):
            part_of[first : first + size] = k
    edge = np.where(part_of[None, :] >= 0, plane[:, cell_of], 0.0)
    edge_hi, edge_lo = halves(edge)
    part = np.broadcast_to(part_of[None, :], (8, 256)).astype(np.int32)
    turn = np.zeros((4, 8, 128), np.float32)
    for s in range(4):
        for r in range(4, 8):
            turn[s, r, :] = b[(r + s) % 4, r % 4]
    pick = np.zeros((192, 256))
    for k in range(3):
        for e in range(64):
            pick[k * 64 + e, lane_of[k, e]] = 1
    pick_hi = pick.astype(BF16)
    pick_lo = np.roll(pick, 64, axis=1).astype(BF16)
    left = np.stack(
        [
            np.concatenate([plane_hi[:192, :256], plane_lo[:192, :256], pick_hi]),
            np.concatenate([plane_hi[192:, 128:], plane_lo[192:, 128:], pick_lo]),
        ]
    )
    whole, gain = whole_basis()
    depth = np.zeros((2, 256, 256))
    place = np.zeros((2, 768, 256))
    for odd in range(2):
        for s in range(16):
            base = 64 * odd + s * LAYERS
            for z in range(LAYERS):
                for o in range(z // 4 * 4, z // 4 * 4 + 4):
                    depth[odd, s * 16 + z, base + o] = whole[z % 4, o % 4]
            for k in range(3):
                for r in range(4):
                    place[odd, k * 256 + s * 16 + 12 + r, base + k * 4 + r] = 1
    lift = np.broadcast_to(np.where(np.arange(256) % 2, gain, 1.0)[None, :], (8, 256)).astype(np.float32)
    column = np.arange(CELLS)
    spread = column[:, None] % 24 == (column[None, :] // CY // 4) * 6 + column[None, :] % CY // 4
    spread = np.stack([spread[:256], spread[128:]]).astype(BF16)
    return (
        spread,
        np.concatenate([edge_hi, edge_lo], axis=1),
        part,
        turn,
        left,
        lift,
        depth.astype(BF16),
        place.astype(BF16),
    )


def dot(a, b):
    return lax.dot_general(a, b, (((1,), (0,)), ((), ())), preferred_element_type=F32)


def dot_rows(a, b):
    return lax.dot_general(a, b, (((1,), (1,)), ((), ())), preferred_element_type=F32)


def two(x):
    hi = x.astype(BF16)
    return hi, (x - hi.astype(F32)).astype(BF16)


def position():
    i, j = lax.axis_index("px"), lax.axis_index("py")
    return ((j >> 1) & 1) * 2 + (i & 1), i >> 1, j >> 2, j & 1


def orders():
    every = [(i, j, k, m) for k in range(4) for j in range(4) for i in range(4) for m in range(2)]
    every = every[1:] if every[0] == (0, 0, 0, 0) else every
    random.Random(0).shuffle(every)
    every.sort(key=lambda d: -sum(min(v, 4 - v) for v in d[:3]))
    return [[d for d in every if d[0] % 2 == phase % 2 and d[1] % 2 == phase // 2] for phase in range(4)]


def half_of(distance):
    return (-distance[1] % 4 - distance[1] % 2) // 2


class Peers:
    def __init__(self):
        x, y, z, c = position()
        xs = [(x + d) & 3 for d in range(4)]
        self.x_low = [v & 1 for v in xs]
        self.x_high = [v & 2 for v in xs]
        self.y_part = [((y + d) & 3) * 2 for d in range(4)]
        self.z = z
        self.y = y
        self.core = [c, 1 - c]

    def z_part(self, d):
        return ((self.z + d) & 3) * 4

    def at(self, dx, dy, dz, dc):
        y = self.y_part[dy] if isinstance(dy, int) else ((self.y + dy) & 3) * 2
        return y + self.x_low[dx], self.z_part(dz) + self.x_high[dx] + self.core[dc]


def ident(pair):
    return {"px": pair[0], "py": pair[1]}


def kernel(
    coef_hbm, expo_hbm, right_hbm, spread_hbm, edge_hbm, part_hbm, turn_hbm, left_hbm, lift_hbm, depth_hbm, place_hbm,
    dec_ref, res_ref, sum_ref,
    coef, expo, right, spread, edge, part_of, turn, left, lift, depth, place,
    sbuf, rbuf, ebuf, dpad, ext, pair_out, pair_in, part, parts,
    load_sem, send_sem, recv_sem, pair_send, pair_recv, sum_send, sum_recv,
):
    x, y, z, c = position()
    peers = Peers()
    me = lax.axis_index("px") * 16 + lax.axis_index("py")
    def load(n, src, dst):
        return pltpu.make_async_copy(src, dst, load_sem.at[n])

    chunks = [
        load(n, coef_hbm.at[:, pl.ds(n * CHUNK, CHUNK)], coef.at[:, pl.ds(n * CHUNK, CHUNK)])
        for n in range(4)
    ]
    first = [load(4, expo_hbm, expo), load(5, spread_hbm, spread)]
    second = [load(6, edge_hbm, edge), load(7, part_hbm, part_of), load(8, turn_hbm, turn)]
    third = [load(9, left_hbm, left), load(10, depth_hbm, depth), load(11, place_hbm, place)]
    third += [load(12, lift_hbm, lift), load(13, right_hbm, right)]
    for copy in [*first, *chunks, *second]:
        copy.start()

    entry = pltpu.get_barrier_semaphore()
    def everywhere(act):
        for distance in sorted(sum(orders(), []), key=lambda d: -sum(min(v, 4 - v) for v in d[:3])):
            act(ident(peers.at(*distance)))

    with jax.named_scope("s_signal"):
        everywhere(lambda there: pl.semaphore_signal(entry, inc=1, device_id=there, device_id_type=MESH))

    def clear(g, _):
        sbuf[pl.ds(g * 16, 16), 8:16, :] = jnp.zeros((16, 8, CELLS), BF16)
        ebuf[g + 1, 0] = jnp.zeros((8, 256), F32)
        ebuf[g + 1, 17] = jnp.zeros((8, 256), F32)
        return 0

    lax.fori_loop(0, 8, clear, 0)
    ebuf[0] = jnp.zeros((18, 8, 256), F32)
    ebuf[9] = jnp.zeros((18, 8, 256), F32)

    with jax.named_scope("s_load"):
        for copy in first:
            copy.wait()

    row8 = lax.broadcasted_iota(jnp.int32, (8, 256), 0)
    lane8 = lax.broadcasted_iota(jnp.int32, (8, 256), 1)
    row12 = lax.broadcasted_iota(jnp.int32, (LAYERS, CELLS), 0)
    owners = (lane8 // 24, (lane8 + 128) // 24)
    upper = lax.broadcasted_iota(jnp.int32, (16, 8, 256), 1) < 4

    def scale(h):
        factors = []
        for n in range(2):
            apart = []
            for g in (2 * h, 2 * h + 1):
                at = g * 384 + n * 128
                power = jnp.exp2(expo[:, at : at + 256].astype(F32))
                rows = jnp.where(row8 % 4 == 0, power[0:1], jnp.where(row8 % 4 == 1, power[1:2], power[2:3]))
                apart += [jnp.where(owners[n] == n * 8 + j + row8 // 4, rows, 0.0) for j in range(0, 8, 2)]
            factors.append(dot(jnp.concatenate(apart, axis=0).astype(BF16), spread[n]))
        for j in range(32):
            at = (h * 32 + j) * CELLS
            held = coef[:, at : at + CELLS].astype(F32)
            row = (j // 16 * 8 + j % 8) * 4
            some = factors[j // 8 % 2][row : row + 3]
            factor = jnp.where(row12 < 4, some[0:1], jnp.where(row12 < 8, some[1:2], some[2:3]))
            sbuf[h * 32 + j, 0:LAYERS, :] = (held * factor).astype(BF16)

    def edges(h):
        held = sbuf[h * 32 : h * 32 + 32].reshape(512, CELLS)
        both = dot(held, edge[...])
        both = (both[:, :256] + both[:, 256:]).reshape(32, ROWS, 256)
        kind = part_of[...][None]
        weights = [jnp.concatenate([turn[s], turn[s]], axis=1)[None] for s in range(4)]
        for n in range(2):
            wide = both[n * 16 : n * 16 + 16]
            first, second = wide[:, :8], wide[:, 8:]
            first_turned, second_turned = pltpu.roll(first, 4, 1), pltpu.roll(second, 4, 1)
            four = jnp.where(
                kind == 0,
                jnp.where(upper, first, first_turned),
                jnp.where(
                    kind == 1, jnp.where(upper, first_turned, first), jnp.where(upper, second, second_turned)
                ),
            )
            mixed = four * weights[0]
            for s in range(1, 4):
                mixed = mixed + pltpu.roll(four, 8 - s, 1) * weights[s]
            ebuf[h * 2 + n + 1, 1:17] = mixed

    with jax.named_scope("s_scale"):
        for h in range(4):
            chunks[h].wait()
            scale(h)

    for copy in third:
        copy.start()
    for copy in second:
        copy.wait()

    with jax.named_scope("s_edges"):
        for h in range(4):
            edges(h)

    lane = lax.broadcasted_iota(jnp.int32, (16, 8, 256), 2)
    low = lane % 48 < 24
    across = lane < 144
    half = lax.broadcasted_iota(jnp.int32, (16, 8, 128), 2) < 64
    even = lax.broadcasted_iota(jnp.int32, (16, 8, 128), 0) % 2 == 0

    def layer(parity, k):
        return (y + parity + 2 * k) & 3

    def gather(g):
        value = jnp.where(low, ebuf[g + 2, 1:17], ebuf[g, 1:17])
        along = jnp.where(even, pltpu.roll(ebuf[g + 1, 0:16, :, 128:], 80, 2), ebuf[g + 1, 2:18, :, 128:])
        one = value[:, :, :128]
        two_ = jnp.where(across[:, :, 128:], value[:, :, 128:], along)
        one_hi = one.astype(BF16).astype(F32)
        two_hi = two_.astype(BF16).astype(F32)
        first = pltpu.roll(one - one_hi, 64, 2)
        second = pltpu.roll(two_ - two_hi, 64, 2)
        line = jnp.concatenate([one_hi, jnp.where(half, two_hi, first), jnp.where(half, first, second)], axis=2)
        tall = jnp.concatenate([jnp.zeros((16, 8, CELLS), F32), line], axis=1).astype(BF16)
        sbuf[pl.ds(g * 16, 16)] = sbuf[pl.ds(g * 16, 16)] + tall

    def collect(phase):
        for k in range(2):
            gather(layer(phase // 2, k) * 2 + ((x + phase) & 1))

    def start(phase):
        for distance in orders()[phase]:
            there = peers.at(*distance)
            pltpu.make_async_remote_copy(
                sbuf.at[there[0] * 16 + there[1]], rbuf.at[me], send_sem, recv_sem.at[phase * 2 + half_of(distance)],
                device_id=ident(there), device_id_type=MESH,
            ).start()

    with jax.named_scope("s_gather"):
        for phase in range(4):
            collect(phase)
    with jax.named_scope("s_bar"):
        pl.semaphore_wait(entry, PEERS - 1)
    with jax.named_scope("s_start"):
        for phase in range(4):
            start(phase)
    rbuf[me] = sbuf[me]

    for copy in third:
        copy.wait()

    def wipe(n, _):
        dpad[n] = jnp.zeros((CY, NZ + 256), F32)
        return 0

    lax.fori_loop(0, CX + 2, wipe, 0)
    ext[...] = jnp.zeros((CX, NZ), F32)

    here = ident(peers.at(0, 0, 0, 1))

    def pair_copy(parity, k):
        at = pl.multiple_of(layer(parity, k) * 384, 128)
        n = parity * 2 + k
        return pltpu.make_async_remote_copy(
            pair_out.at[:, pl.ds(at, 384)], pair_in.at[:, pl.ds(at, 384)], pair_send.at[n], pair_recv.at[n],
            device_id=here, device_id_type=MESH,
        )

    def pair_start(parity, k):
        at = layer(parity, k) * 384
        lanes = pl.ds(pl.multiple_of(at + 128, 128), 384)
        last = dpad[1 : CX + 1, CY - 8 :, lanes][:, 7, :]
        first = dpad[1 : CX + 1, 0:8, lanes][:, 0, :]
        pair_out[:, pl.ds(pl.multiple_of(at, 128), 384)] = jnp.where(c == 0, last, first)
        pair_copy(parity, k).start()

    def decode(phase, ks):
        odd = (x + phase) & 1
        wides = []
        for k in ks:
            held = rbuf[pl.ds((layer(phase // 2, k) * 2 + odd) * 16, 16)].reshape(256, CELLS)
            wides.append((dot_rows(left[0], held[:, :256]), dot_rows(left[1], held[:, 128:])))
        for k, (near, far) in zip(ks, wides):
            across = jnp.concatenate([near[:192] + near[192:384], far[:192] + far[192:384]], axis=0)
            hi, lo = two(across * lift[0:1, :])
            field = dot(hi, depth[odd]) + dot(lo, depth[odd])
            side_hi = jnp.concatenate([near[384:448], near[448:512], near[512:576]], axis=1).astype(BF16)
            side_lo = jnp.concatenate([far[384:448], far[448:512], far[512:576]], axis=1).astype(BF16)
            side = dot(jnp.concatenate([side_hi, side_lo], axis=0), place[odd])
            side = side[:64] + side[64:]
            at = layer(phase // 2, k) * 384 + odd * 128
            lanes = pl.ds(pl.multiple_of(at + 128, 128), 256)
            dpad[1 : CX + 1, :, lanes] += field.reshape(CX, CY, 256)
            dpad[0, :, lanes] += side[24:48]
            dpad[CX + 1, :, lanes] += side[0:24]
            ext[:, pl.ds(pl.multiple_of(at, 128), 256)] += side[48:64]
            if phase % 2 == 1:
                pair_start(phase // 2, k)

    column = lax.broadcasted_iota(jnp.int32, (CY, 384), 1)
    row = lax.broadcasted_iota(jnp.int32, (CY, 384), 0)
    tile = lax.broadcasted_iota(jnp.int32, (CY, 128), 1)

    def squares(value):
        value = value * value
        value = value[0:8] + value[8:16] + value[16:24]
        return sum(value[:, k * 128 : (k + 1) * 128] for k in range(value.shape[1] // 128))

    def residual(parity, k, total):
        depth_at = layer(parity, k)
        at = depth_at * 384
        lanes = pl.ds(pl.multiple_of(at, 128), 384)
        inside = pl.ds(pl.multiple_of(at + 128, 128), 384)
        low_at = jnp.maximum(at - 128, 0)
        high_at = jnp.minimum(at + 384, NZ - 128)
        counted = ((column > 0) | (depth_at == 0)) & ((column < 383) | (depth_at == 3))

        def slab(n, total):
            rows = pl.ds(pl.multiple_of(n * CY, 8), CY)
            own = dpad[n + 1, :, inside]
            near = dpad[n, :, inside] + dpad[n + 2, :, inside]
            inner, outer = pair_in[pl.ds(n, 1), lanes], ext[pl.ds(n, 1), lanes]
            below = jnp.where(c == 0, outer, inner)
            above = jnp.where(c == 0, inner, outer)
            near = near + jnp.where(row == 0, below, pltpu.roll(own, 1, 0))
            near = near + jnp.where(row == CY - 1, above, pltpu.roll(own, CY - 1, 0))
            back, forth = pltpu.roll(own, 1, 1), pltpu.roll(own, 383, 1)
            if parity == 0:
                back = jnp.where(column == 0, 0.0, back)
                forth = jnp.where(column == 383, 0.0, forth)
            else:
                prior = dpad[n + 1, :, pl.ds(pl.multiple_of(at, 128), 128)]
                later = dpad[n + 1, :, pl.ds(pl.multiple_of(at + 512, 128), 128)]
                first, last = back[:, :128], forth[:, 256:]
                back = jnp.concatenate([jnp.where(tile == 0, pltpu.roll(prior, 1, 1), first), back[:, 128:]], axis=1)
                forth = jnp.concatenate(
                    [forth[:, :256], jnp.where(tile == 127, pltpu.roll(later, 127, 1), last)], axis=1
                )
            value = right[rows, lanes] - (6.0 * own - (near + back + forth))
            dec_ref[rows, lanes] = own
            res_ref[rows, lanes] = value
            if parity == 0:
                return total + squares(jnp.where(counted, value, 0.0))
            total = total + squares(value)
            for there, edge_lane, carried, exists in (
                (low_at, 127, last, depth_at > 0),
                (high_at, 0, first, depth_at < 3),
            ):
                spot = pl.ds(pl.multiple_of(there, 128), 128)
                mine = (tile == edge_lane) & exists
                value = res_ref[rows, spot] + jnp.where(mine, carried, 0.0)
                res_ref[rows, spot] = value
                total = total + squares(jnp.where(mine, value, 0.0))
            return total

        return lax.fori_loop(0, CX, slab, total, unroll=8)

    total = jnp.zeros((8, 128), F32)
    for phase in range(4):
        def arrive(k):
            block = rbuf.at[pl.ds(0, 16 - (phase == 0 and k == 0))]
            with jax.named_scope("s_wait"):
                pltpu.make_async_copy(block, block, recv_sem.at[phase * 2 + k]).wait()

        if phase == 3:
            arrive(0)
            arrive(1)
            with jax.named_scope("s_decode"):
                decode(phase, (0, 1))
        else:
            for k in range(2):
                arrive(k)
                with jax.named_scope("s_decode"):
                    decode(phase, (k,))
        if phase == 1:
            with jax.named_scope("s_early"):
                for k in range(2):
                    pair_copy(0, k).wait()
                    total = residual(0, k, total)
    for k in range(2):
        with jax.named_scope("s_pair"):
            pair_copy(1, k).wait()
        with jax.named_scope("s_late"):
            total = residual(1, k, total)

    part[...] = jnp.sum(total, axis=0, keepdims=True)
    parts[me] = part[...]

    everyone = pl.ds(0, PEERS - 1)
    with jax.named_scope("s_sent"):
        pltpu.make_async_copy(sbuf.at[everyone], sbuf.at[everyone], send_sem).wait()
    with jax.named_scope("s_tell"):
        everywhere(
            lambda there: pltpu.make_async_remote_copy(
                part, parts.at[me], sum_send, sum_recv, device_id=there, device_id_type=MESH
            ).start()
        )
    with jax.named_scope("s_sum"):
        pltpu.make_async_copy(parts.at[everyone], parts.at[everyone], sum_recv).wait()
    pltpu.make_async_copy(parts.at[everyone], parts.at[everyone], sum_send).wait()
    sum_ref[...] = jnp.broadcast_to(jnp.sum(parts[...], axis=0), (8, 128))


def deliver(dec_ref, res_ref, sum_ref, dec_out, res_out, rms_out, rms, sems):
    copies = [
        pltpu.make_async_copy(src, dst, sems.at[n])
        for n, (src, dst) in enumerate(((dec_ref, dec_out), (res_ref, res_out), (rms, rms_out)))
    ]
    copies[0].start()
    copies[1].start()
    whole = jnp.sum(sum_ref[0:1, :], axis=1, keepdims=True)
    rms[...] = jnp.sqrt(whole / (PEERS * CELLS * NZ) + 1e-06)
    copies[2].start()
    for copy in copies:
        copy.wait()


def shards(coefficients, exponents, right_side):
    constants = tables()
    any_space = pl.BlockSpec(memory_space=pltpu.HBM)
    vmem = pl.BlockSpec(memory_space=pltpu.VMEM)
    right = right_side.reshape(CELLS, NZ)
    operands = (coefficients, exponents, right, *constants)
    operands = tuple(pltpu.with_memory_space_constraint(jnp.asarray(o), pltpu.HBM) for o in operands)
    held = [pltpu.VMEM(o.shape, o.dtype) for o in operands]
    sem = pltpu.SemaphoreType
    field = jax.ShapeDtypeStruct((CELLS, NZ), F32)
    decoded, residual, total = pl.pallas_call(
        kernel,
        name="exchange",
        out_shape=(field, field, jax.ShapeDtypeStruct((8, 128), F32)),
        in_specs=[any_space] * len(operands),
        out_specs=(vmem, vmem, vmem),
        scratch_shapes=[
            *held,
            pltpu.VMEM((PEERS, ROWS, CELLS), BF16),
            pltpu.VMEM((PEERS, ROWS, CELLS), BF16),
            pltpu.VMEM((10, 18, 8, 256), F32),
            pltpu.VMEM((CX + 2, CY, NZ + 256), F32),
            pltpu.VMEM((CX, NZ), F32),
            pltpu.VMEM((CX, NZ), F32),
            pltpu.VMEM((CX, NZ), F32),
            pltpu.VMEM((1, 128), F32),
            pltpu.VMEM((PEERS, 1, 128), F32),
            sem.DMA((14,)),
            sem.DMA,
            sem.DMA((8,)),
            sem.DMA((4,)),
            sem.DMA((4,)),
            sem.DMA,
            sem.DMA,
        ],
        compiler_params=pltpu.CompilerParams(collective_id=0, has_side_effects=True, vmem_limit_bytes=VMEM_BYTES),
    )(*operands)
    shape = (CX, CY, NZ)
    decoded, residual, rms = pl.pallas_call(
        deliver,
        name="deliver",
        out_shape=(field, field, jax.ShapeDtypeStruct((1, 1), F32)),
        in_specs=(vmem, vmem, vmem),
        out_specs=(any_space, any_space, any_space),
        scratch_shapes=[pltpu.VMEM((1, 1), F32), sem.DMA((3,))],
        compiler_params=pltpu.CompilerParams(vmem_limit_bytes=1 << 20),
    )(decoded, residual, total)
    return decoded.reshape(shape), residual.reshape(shape), rms[0, 0]


def solution(mesh):
    placed = (P(("px", "py"), None), P(("px", "py"), None), P("px", "py", None))
    return jax.shard_map(
        shards,
        mesh=mesh,
        in_specs=placed,
        out_specs=(P("px", "py", None), P("px", "py", None), P()),
        check_vma=False,
    )
```

```python
import random

import jax
import jax.numpy as jnp
import numpy as np
from jax import lax
from jax.experimental import pallas as pl
from jax.experimental.pallas import tpu as pltpu
from jax.sharding import PartitionSpec as P

CX = 16
CY = 24
CELLS = CX * CY
NZ = 1536
PEERS = 128
LAYERS = 12
CHUNK = CELLS * PEERS // 4
ROWS = 16
F32 = jnp.float32
BF16 = jnp.bfloat16
MESH = pl.DeviceIdType.MESH
VMEM_BYTES = 40 << 20


def basis():
    a = np.arange(4.0)[:, None]
    i = np.arange(4.0)[None, :]
    weight = np.where(a == 0, np.sqrt(0.25), np.sqrt(0.5))
    return weight * np.cos(np.pi * (2 * i + 1) * a / 8)


def halves(table):
    hi = table.astype(np.float32).astype(BF16)
    lo = (table - hi.astype(np.float64)).astype(np.float32).astype(BF16)
    return hi, lo


def whole_basis():
    b = basis()
    p, q = 408 / 512, 169 / 512
    gain = np.sqrt(b[1, 0] / p * b[1, 1] / q)
    return np.stack([b[0], [p, q, -q, -p], b[2], [q, -p, p, -q]]), gain


def block_table(width):
    b = basis()
    n = np.arange(width)
    return np.where(n[:, None] // 4 == n[None, :] // 4, b[n[:, None] % 4, n[None, :] % 4], 0.0)


def tables():
    b = basis()
    plane = np.kron(block_table(CX), block_table(CY))
    plane_hi, plane_lo = halves(plane.T)
    lane_of = np.zeros((3, 64), np.int64)
    cell_of = np.zeros(256, np.int64)
    part_of = np.full(256, -1)
    for k in range(3):
        for e in range(64):
            lane_of[k, e] = k * 48 + e if e < 48 else 144 + k * 16 + e - 48
        for e in range(24):
            cell_of[k * 48 + e] = e
            cell_of[k * 48 + 24 + e] = 15 * CY + e
        for x in range(16):
            cell_of[144 + k * 16 + x] = x * CY
            cell_of[192 + k * 16 + x] = x * CY + 23
        for first, size in ((k * 48, 48), (144 + k * 16, 16), (192 + k * 16, 16)):
            part_of[first : first + size] = k
    edge = np.where(part_of[None, :] >= 0, plane[:, cell_of], 0.0)
    edge_hi, edge_lo = halves(edge)
    part = np.broadcast_to(part_of[None, :], (8, 256)).astype(np.int32)
    turn = np.zeros((4, 8, 128), np.float32)
    for s in range(4):
        for r in range(4, 8):
            turn[s, r, :] = b[(r + s) % 4, r % 4]
    pick = np.zeros((192, 256))
    for k in range(3):
        for e in range(64):
            pick[k * 64 + e, lane_of[k, e]] = 1
    pick_hi = pick.astype(BF16)
    pick_lo = np.roll(pick, 64, axis=1).astype(BF16)
    left = np.stack(
        [
            np.concatenate([plane_hi[:192, :256], plane_lo[:192, :256], pick_hi]),
            np.concatenate([plane_hi[192:, 128:], plane_lo[192:, 128:], pick_lo]),
        ]
    )
    whole, gain = whole_basis()
    depth = np.zeros((2, 256, 256))
    place = np.zeros((2, 768, 256))
    for odd in range(2):
        for s in range(16):
            base = 64 * odd + s * LAYERS
            for z in range(LAYERS):
                for o in range(z // 4 * 4, z // 4 * 4 + 4):
                    depth[odd, s * 16 + z, base + o] = whole[z % 4, o % 4]
            for k in range(3):
                for r in range(4):
                    place[odd, k * 256 + s * 16 + 12 + r, base + k * 4 + r] = 1
    lift = np.broadcast_to(np.where(np.arange(256) % 2, gain, 1.0)[None, :], (8, 256)).astype(np.float32)
    column = np.arange(CELLS)
    spread = column[:, None] % 24 == (column[None, :] // CY // 4) * 6 + column[None, :] % CY // 4
    spread = np.stack([spread[:256], spread[128:]]).astype(BF16)
    return (
        spread,
        np.concatenate([edge_hi, edge_lo], axis=1),
        part,
        turn,
        left,
        lift,
        depth.astype(BF16),
        place.astype(BF16),
    )


def dot(a, b):
    return lax.dot_general(a, b, (((1,), (0,)), ((), ())), preferred_element_type=F32)


def dot_rows(a, b):
    return lax.dot_general(a, b, (((1,), (1,)), ((), ())), preferred_element_type=F32)


def two(x):
    hi = x.astype(BF16)
    return hi, (x - hi.astype(F32)).astype(BF16)


def position():
    i, j = lax.axis_index("px"), lax.axis_index("py")
    return ((j >> 1) & 1) * 2 + (i & 1), i >> 1, j >> 2, j & 1


def orders():
    every = [(i, j, k, m) for k in range(4) for j in range(4) for i in range(4) for m in range(2)]
    every = every[1:] if every[0] == (0, 0, 0, 0) else every
    random.Random(0).shuffle(every)
    every.sort(key=lambda d: -sum(min(v, 4 - v) for v in d[:3]))
    return [[d for d in every if d[0] % 2 == phase % 2 and d[1] % 2 == phase // 2] for phase in range(4)]


def half_of(distance):
    return (-distance[1] % 4 - distance[1] % 2) // 2


class Peers:
    def __init__(self):
        x, y, z, c = position()
        xs = [(x + d) & 3 for d in range(4)]
        self.x_low = [v & 1 for v in xs]
        self.x_high = [v & 2 for v in xs]
        self.y_part = [((y + d) & 3) * 2 for d in range(4)]
        self.z = z
        self.y = y
        self.core = [c, 1 - c]

    def z_part(self, d):
        return ((self.z + d) & 3) * 4

    def at(self, dx, dy, dz, dc):
        y = self.y_part[dy] if isinstance(dy, int) else ((self.y + dy) & 3) * 2
        return y + self.x_low[dx], self.z_part(dz) + self.x_high[dx] + self.core[dc]


def ident(pair):
    return {"px": pair[0], "py": pair[1]}


def kernel(
    coef_hbm, expo_hbm, right_hbm, spread_hbm, edge_hbm, part_hbm, turn_hbm, left_hbm, lift_hbm, depth_hbm, place_hbm,
    dec_ref, res_ref, sum_ref,
    coef, expo, right, spread, edge, part_of, turn, left, lift, depth, place,
    sbuf, rbuf, ebuf, dpad, ext, pair_out, pair_in, part, parts,
    load_sem, send_sem, recv_sem, pair_send, pair_recv, sum_send, sum_recv,
):
    x, y, z, c = position()
    peers = Peers()
    me = lax.axis_index("px") * 16 + lax.axis_index("py")
    def load(n, src, dst):
        return pltpu.make_async_copy(src, dst, load_sem.at[n])

    chunks = [
        load(n, coef_hbm.at[:, pl.ds(n * CHUNK, CHUNK)], coef.at[:, pl.ds(n * CHUNK, CHUNK)])
        for n in range(4)
    ]
    first = [load(4, expo_hbm, expo), load(5, spread_hbm, spread)]
    second = [load(6, edge_hbm, edge), load(7, part_hbm, part_of), load(8, turn_hbm, turn)]
    third = [load(9, left_hbm, left), load(10, depth_hbm, depth), load(11, place_hbm, place)]
    third += [load(12, lift_hbm, lift), load(13, right_hbm, right)]

    entry = pltpu.get_barrier_semaphore()
    def hops(distance):
        return sum(min(v, 4 - v) for v in distance[:3])

    def everywhere(act, least=0, most=6):
        for distance in sorted(sum(orders(), []), key=lambda d: -hops(d)):
            if least <= hops(distance) <= most:
                act(ident(peers.at(*distance)))

    def greet(there):
        pl.semaphore_signal(entry, inc=1, device_id=there, device_id_type=MESH)

    with jax.named_scope("s_signal"):
        everywhere(greet, 5, 6)
        for copy in [*first, *chunks]:
            copy.start()
        everywhere(greet, 0, 4)
        for copy in second:
            copy.start()

    def clear(g, _):
        sbuf[pl.ds(g * 16, 16), 8:16, :] = jnp.zeros((16, 8, CELLS), BF16)
        ebuf[g + 1, 0] = jnp.zeros((8, 256), F32)
        ebuf[g + 1, 17] = jnp.zeros((8, 256), F32)
        return 0

    lax.fori_loop(0, 8, clear, 0)
    ebuf[0] = jnp.zeros((18, 8, 256), F32)
    ebuf[9] = jnp.zeros((18, 8, 256), F32)

    with jax.named_scope("s_load"):
        for copy in first:
            copy.wait()

    row8 = lax.broadcasted_iota(jnp.int32, (8, 256), 0)
    lane8 = lax.broadcasted_iota(jnp.int32, (8, 256), 1)
    row12 = lax.broadcasted_iota(jnp.int32, (LAYERS, CELLS), 0)
    owners = (lane8 // 24, (lane8 + 128) // 24)
    upper = lax.broadcasted_iota(jnp.int32, (16, 8, 256), 1) < 4

    def scale(h):
        factors = []
        for n in range(2):
            apart = []
            for g in (2 * h, 2 * h + 1):
                at = g * 384 + n * 128
                power = jnp.exp2(expo[:, at : at + 256].astype(F32))
                rows = jnp.where(row8 % 4 == 0, power[0:1], jnp.where(row8 % 4 == 1, power[1:2], power[2:3]))
                apart += [jnp.where(owners[n] == n * 8 + j + row8 // 4, rows, 0.0) for j in range(0, 8, 2)]
            factors.append(dot(jnp.concatenate(apart, axis=0).astype(BF16), spread[n]))
        for j in range(32):
            at = (h * 32 + j) * CELLS
            held = coef[:, at : at + CELLS].astype(F32)
            row = (j // 16 * 8 + j % 8) * 4
            some = factors[j // 8 % 2][row : row + 3]
            factor = jnp.where(row12 < 4, some[0:1], jnp.where(row12 < 8, some[1:2], some[2:3]))
            sbuf[h * 32 + j, 0:LAYERS, :] = (held * factor).astype(BF16)

    def edges(h):
        held = sbuf[h * 32 : h * 32 + 32].reshape(512, CELLS)
        both = dot(held, edge[...])
        both = (both[:, :256] + both[:, 256:]).reshape(32, ROWS, 256)
        kind = part_of[...][None]
        weights = [jnp.concatenate([turn[s], turn[s]], axis=1)[None] for s in range(4)]
        for n in range(2):
            wide = both[n * 16 : n * 16 + 16]
            first, second = wide[:, :8], wide[:, 8:]
            first_turned, second_turned = pltpu.roll(first, 4, 1), pltpu.roll(second, 4, 1)
            four = jnp.where(
                kind == 0,
                jnp.where(upper, first, first_turned),
                jnp.where(
                    kind == 1, jnp.where(upper, first_turned, first), jnp.where(upper, second, second_turned)
                ),
            )
            mixed = four * weights[0]
            for s in range(1, 4):
                mixed = mixed + pltpu.roll(four, 8 - s, 1) * weights[s]
            ebuf[h * 2 + n + 1, 1:17] = mixed

    with jax.named_scope("s_scale"):
        for h in range(4):
            chunks[h].wait()
            scale(h)

    for copy in third:
        copy.start()
    for copy in second:
        copy.wait()

    with jax.named_scope("s_edges"):
        for h in range(4):
            edges(h)

    lane = lax.broadcasted_iota(jnp.int32, (16, 8, 256), 2)
    low = lane % 48 < 24
    across = lane < 144
    half = lax.broadcasted_iota(jnp.int32, (16, 8, 128), 2) < 64
    even = lax.broadcasted_iota(jnp.int32, (16, 8, 128), 0) % 2 == 0

    def layer(parity, k):
        return (y + parity + 2 * k) & 3

    def gather(g):
        value = jnp.where(low, ebuf[g + 2, 1:17], ebuf[g, 1:17])
        along = jnp.where(even, pltpu.roll(ebuf[g + 1, 0:16, :, 128:], 80, 2), ebuf[g + 1, 2:18, :, 128:])
        one = value[:, :, :128]
        two_ = jnp.where(across[:, :, 128:], value[:, :, 128:], along)
        one_hi = one.astype(BF16).astype(F32)
        two_hi = two_.astype(BF16).astype(F32)
        first = pltpu.roll(one - one_hi, 64, 2)
        second = pltpu.roll(two_ - two_hi, 64, 2)
        line = jnp.concatenate([one_hi, jnp.where(half, two_hi, first), jnp.where(half, first, second)], axis=2)
        tall = jnp.concatenate([jnp.zeros((16, 8, CELLS), F32), line], axis=1).astype(BF16)
        sbuf[pl.ds(g * 16, 16)] = sbuf[pl.ds(g * 16, 16)] + tall

    def collect(phase):
        for k in range(2):
            gather(layer(phase // 2, k) * 2 + ((x + phase) & 1))

    def start(phase):
        for distance in orders()[phase]:
            there = peers.at(*distance)
            pltpu.make_async_remote_copy(
                sbuf.at[there[0] * 16 + there[1]], rbuf.at[me], send_sem, recv_sem.at[phase * 2 + half_of(distance)],
                device_id=ident(there), device_id_type=MESH,
            ).start()

    with jax.named_scope("s_gather"):
        for phase in range(4):
            collect(phase)
    with jax.named_scope("s_bar"):
        pl.semaphore_wait(entry, PEERS - 1)
    with jax.named_scope("s_start"):
        for phase in range(4):
            start(phase)
    rbuf[me] = sbuf[me]

    for copy in third:
        copy.wait()

    def wipe(n, _):
        dpad[n] = jnp.zeros((CY, NZ + 256), F32)
        return 0

    lax.fori_loop(0, CX + 2, wipe, 0)
    ext[...] = jnp.zeros((CX, NZ), F32)

    here = ident(peers.at(0, 0, 0, 1))

    def pair_copy(parity, k):
        at = pl.multiple_of(layer(parity, k) * 384, 128)
        n = parity * 2 + k
        return pltpu.make_async_remote_copy(
            pair_out.at[:, pl.ds(at, 384)], pair_in.at[:, pl.ds(at, 384)], pair_send.at[n], pair_recv.at[n],
            device_id=here, device_id_type=MESH,
        )

    def pair_start(parity, k):
        at = layer(parity, k) * 384
        lanes = pl.ds(pl.multiple_of(at + 128, 128), 384)
        last = dpad[1 : CX + 1, CY - 8 :, lanes][:, 7, :]
        first = dpad[1 : CX + 1, 0:8, lanes][:, 0, :]
        pair_out[:, pl.ds(pl.multiple_of(at, 128), 384)] = jnp.where(c == 0, last, first)
        pair_copy(parity, k).start()

    def decode(phase, ks):
        odd = (x + phase) & 1
        wides = []
        for k in ks:
            held = rbuf[pl.ds((layer(phase // 2, k) * 2 + odd) * 16, 16)].reshape(256, CELLS)
            wides.append((dot_rows(left[0], held[:, :256]), dot_rows(left[1], held[:, 128:])))
        for k, (near, far) in zip(ks, wides):
            across = jnp.concatenate([near[:192] + near[192:384], far[:192] + far[192:384]], axis=0)
            hi, lo = two(across * lift[0:1, :])
            field = dot(hi, depth[odd]) + dot(lo, depth[odd])
            side_hi = jnp.concatenate([near[384:448], near[448:512], near[512:576]], axis=1).astype(BF16)
            side_lo = jnp.concatenate([far[384:448], far[448:512], far[512:576]], axis=1).astype(BF16)
            side = dot(jnp.concatenate([side_hi, side_lo], axis=0), place[odd])
            side = side[:64] + side[64:]
            at = layer(phase // 2, k) * 384 + odd * 128
            lanes = pl.ds(pl.multiple_of(at + 128, 128), 256)
            dpad[1 : CX + 1, :, lanes] += field.reshape(CX, CY, 256)
            dpad[0, :, lanes] += side[24:48]
            dpad[CX + 1, :, lanes] += side[0:24]
            ext[:, pl.ds(pl.multiple_of(at, 128), 256)] += side[48:64]
            if phase % 2 == 1:
                pair_start(phase // 2, k)

    column = lax.broadcasted_iota(jnp.int32, (CY, 384), 1)
    row = lax.broadcasted_iota(jnp.int32, (CY, 384), 0)
    tile = lax.broadcasted_iota(jnp.int32, (CY, 128), 1)

    def squares(value):
        value = value * value
        value = value[0:8] + value[8:16] + value[16:24]
        return sum(value[:, k * 128 : (k + 1) * 128] for k in range(value.shape[1] // 128))

    def residual(parity, k, total):
        depth_at = layer(parity, k)
        at = depth_at * 384
        lanes = pl.ds(pl.multiple_of(at, 128), 384)
        inside = pl.ds(pl.multiple_of(at + 128, 128), 384)
        low_at = jnp.maximum(at - 128, 0)
        high_at = jnp.minimum(at + 384, NZ - 128)
        counted = ((column > 0) | (depth_at == 0)) & ((column < 383) | (depth_at == 3))

        def slab(n, total):
            rows = pl.ds(pl.multiple_of(n * CY, 8), CY)
            own = dpad[n + 1, :, inside]
            near = dpad[n, :, inside] + dpad[n + 2, :, inside]
            inner, outer = pair_in[pl.ds(n, 1), lanes], ext[pl.ds(n, 1), lanes]
            below = jnp.where(c == 0, outer, inner)
            above = jnp.where(c == 0, inner, outer)
            near = near + jnp.where(row == 0, below, pltpu.roll(own, 1, 0))
            near = near + jnp.where(row == CY - 1, above, pltpu.roll(own, CY - 1, 0))
            back, forth = pltpu.roll(own, 1, 1), pltpu.roll(own, 383, 1)
            if parity == 0:
                back = jnp.where(column == 0, 0.0, back)
                forth = jnp.where(column == 383, 0.0, forth)
            else:
                prior = dpad[n + 1, :, pl.ds(pl.multiple_of(at, 128), 128)]
                later = dpad[n + 1, :, pl.ds(pl.multiple_of(at + 512, 128), 128)]
                first, last = back[:, :128], forth[:, 256:]
                back = jnp.concatenate([jnp.where(tile == 0, pltpu.roll(prior, 1, 1), first), back[:, 128:]], axis=1)
                forth = jnp.concatenate(
                    [forth[:, :256], jnp.where(tile == 127, pltpu.roll(later, 127, 1), last)], axis=1
                )
            value = right[rows, lanes] - (6.0 * own - (near + back + forth))
            dec_ref[rows, lanes] = own
            res_ref[rows, lanes] = value
            if parity == 0:
                return total + squares(jnp.where(counted, value, 0.0))
            total = total + squares(value)
            for there, edge_lane, carried, exists in (
                (low_at, 127, last, depth_at > 0),
                (high_at, 0, first, depth_at < 3),
            ):
                spot = pl.ds(pl.multiple_of(there, 128), 128)
                mine = (tile == edge_lane) & exists
                value = res_ref[rows, spot] + jnp.where(mine, carried, 0.0)
                res_ref[rows, spot] = value
                total = total + squares(jnp.where(mine, value, 0.0))
            return total

        return lax.fori_loop(0, CX, slab, total, unroll=8)

    total = jnp.zeros((8, 128), F32)
    for phase in range(4):
        def arrive(k):
            block = rbuf.at[pl.ds(0, 16 - (phase == 0 and k == 0))]
            with jax.named_scope("s_wait"):
                pltpu.make_async_copy(block, block, recv_sem.at[phase * 2 + k]).wait()

        if phase == 3:
            arrive(0)
            arrive(1)
            with jax.named_scope("s_decode"):
                decode(phase, (0, 1))
        else:
            for k in range(2):
                arrive(k)
                with jax.named_scope("s_decode"):
                    decode(phase, (k,))
        if phase == 1:
            with jax.named_scope("s_early"):
                for k in range(2):
                    pair_copy(0, k).wait()
                    total = residual(0, k, total)
    for k in range(2):
        with jax.named_scope("s_pair"):
            pair_copy(1, k).wait()
        with jax.named_scope("s_late"):
            total = residual(1, k, total)

    part[...] = jnp.sum(total, axis=0, keepdims=True)
    parts[me] = part[...]

    everyone = pl.ds(0, PEERS - 1)
    with jax.named_scope("s_sent"):
        pltpu.make_async_copy(sbuf.at[everyone], sbuf.at[everyone], send_sem).wait()
    with jax.named_scope("s_tell"):
        everywhere(
            lambda there: pltpu.make_async_remote_copy(
                part, parts.at[me], sum_send, sum_recv, device_id=there, device_id_type=MESH
            ).start()
        )
    with jax.named_scope("s_sum"):
        pltpu.make_async_copy(parts.at[everyone], parts.at[everyone], sum_recv).wait()
    pltpu.make_async_copy(parts.at[everyone], parts.at[everyone], sum_send).wait()
    sum_ref[...] = jnp.broadcast_to(jnp.sum(parts[...], axis=0), (8, 128))


def deliver(dec_ref, res_ref, sum_ref, dec_out, res_out, rms_out, rms, sems):
    copies = [
        pltpu.make_async_copy(src, dst, sems.at[n])
        for n, (src, dst) in enumerate(((dec_ref, dec_out), (res_ref, res_out), (rms, rms_out)))
    ]
    copies[0].start()
    copies[1].start()
    whole = jnp.sum(sum_ref[0:1, :], axis=1, keepdims=True)
    rms[...] = jnp.sqrt(whole / (PEERS * CELLS * NZ) + 1e-06)
    copies[2].start()
    for copy in copies:
        copy.wait()


def shards(coefficients, exponents, right_side):
    constants = tables()
    any_space = pl.BlockSpec(memory_space=pltpu.HBM)
    vmem = pl.BlockSpec(memory_space=pltpu.VMEM)
    right = right_side.reshape(CELLS, NZ)
    operands = (coefficients, exponents, right, *constants)
    operands = tuple(pltpu.with_memory_space_constraint(jnp.asarray(o), pltpu.HBM) for o in operands)
    held = [pltpu.VMEM(o.shape, o.dtype) for o in operands]
    sem = pltpu.SemaphoreType
    field = jax.ShapeDtypeStruct((CELLS, NZ), F32)
    decoded, residual, total = pl.pallas_call(
        kernel,
        name="exchange",
        out_shape=(field, field, jax.ShapeDtypeStruct((8, 128), F32)),
        in_specs=[any_space] * len(operands),
        out_specs=(vmem, vmem, vmem),
        scratch_shapes=[
            *held,
            pltpu.VMEM((PEERS, ROWS, CELLS), BF16),
            pltpu.VMEM((PEERS, ROWS, CELLS), BF16),
            pltpu.VMEM((10, 18, 8, 256), F32),
            pltpu.VMEM((CX + 2, CY, NZ + 256), F32),
            pltpu.VMEM((CX, NZ), F32),
            pltpu.VMEM((CX, NZ), F32),
            pltpu.VMEM((CX, NZ), F32),
            pltpu.VMEM((1, 128), F32),
            pltpu.VMEM((PEERS, 1, 128), F32),
            sem.DMA((14,)),
            sem.DMA,
            sem.DMA((8,)),
            sem.DMA((4,)),
            sem.DMA((4,)),
            sem.DMA,
            sem.DMA,
        ],
        compiler_params=pltpu.CompilerParams(collective_id=0, has_side_effects=True, vmem_limit_bytes=VMEM_BYTES),
    )(*operands)
    shape = (CX, CY, NZ)
    decoded, residual, rms = pl.pallas_call(
        deliver,
        name="deliver",
        out_shape=(field, field, jax.ShapeDtypeStruct((1, 1), F32)),
        in_specs=(vmem, vmem, vmem),
        out_specs=(any_space, any_space, any_space),
        scratch_shapes=[pltpu.VMEM((1, 1), F32), sem.DMA((3,))],
        compiler_params=pltpu.CompilerParams(vmem_limit_bytes=1 << 20),
    )(decoded, residual, total)
    return decoded.reshape(shape), residual.reshape(shape), rms[0, 0]


def solution(mesh):
    placed = (P(("px", "py"), None), P(("px", "py"), None), P("px", "py", None))
    return jax.shard_map(
        shards,
        mesh=mesh,
        in_specs=placed,
        out_specs=(P("px", "py", None), P("px", "py", None), P()),
        check_vma=False,
    )
```
